32 devices in a mesh: dp: 4 (over x, y), tp: 8 (over z, core).
Axes of the slice: x: 2, y: 2, z: 4, core: 2. Of those that a mesh axis runs over, the one named last changes fastest.
Arguments:
- X: bfloat16 [1024, 2048], P(('dp', 'tp')), parts along dimension 0
- dY: bfloat16 [1024, 2048], P(('dp', 'tp')), parts along dimension 0
- W1: bfloat16 [2048, 8192], P(None, 'tp')
- W2: bfloat16 [8192, 2048], P('tp')
Outputs:
- output 1: bfloat16 [1024, 2048], P(('dp', 'tp')), parts along dimension 0
- output 2: float32 [8192, 8192], P('dp', 'tp'), parts along dimension 0
- output 3: float32 [32768, 2048], P(('dp', 'tp')), parts along dimension 0
There are 4 independent parts. The reference program is written for one: setup_inputs(seed, part) draws one part's arguments, and reference() takes and returns one part's arrays. A program takes and returns all parts, laid end to end along the dimension named above; an argument that names none is the same for every part.
All inputs are finite; a program needn't handle non-finite values.
Results may differ from the reference program's by a relative error of at most 0.00939837.
Values are sent between devices in bfloat16 or wider.
A program may use at most 1 GiB of HBM per device.

```python
import math
import jax
import jax.numpy as jnp
from jax import lax

TP = 8
TOKENS_DEV = 32
H = 2048
FF_DEV = 1024

T = TOKENS_DEV * TP
F = FF_DEV * TP
C0 = math.sqrt(2.0 / math.pi)
C1 = 0.044715


def _gelu(u):
    t = jnp.tanh(C0 * (u + C1 * u * u * u))
    return 0.5 * u * (1.0 + t), 0.5 * (1.0 + t) + 0.5 * u * (1.0 - t * t) * C0 * (1.0 + 3.0 * C1 * u * u)


def setup_inputs(seed: int = 0, part: int = 0) -> dict:
    key = jax.random.PRNGKey(seed)
    ks = jax.random.split(key, 3)
    kx, kdy = jax.random.split(jax.random.fold_in(ks[0], part))
    x = jax.random.normal(kx, (T, H), jnp.float32).astype(jnp.bfloat16)
    dy = jax.random.normal(kdy, (T, H), jnp.float32).astype(jnp.bfloat16)
    w1 = (jax.random.normal(ks[1], (H, F), jnp.float32) * H ** -0.5).astype(jnp.bfloat16)
    w2 = (jax.random.normal(ks[2], (F, H), jnp.float32) * F ** -0.5).astype(jnp.bfloat16)
    return {'X': x, 'dY': dy, 'W1': w1, 'W2': w2}


def reference(X, dY, W1, W2):
    w1c = W1.reshape(H, TP, FF_DEV).transpose(1, 0, 2)
    w2c = W2.reshape(TP, FF_DEV, H)

    def step(acc, w):
        a, b = w
        u = jnp.dot(X, a, preferred_element_type=jnp.float32).astype(jnp.bfloat16)
        g0, g1 = _gelu(u.astype(jnp.float32))
        z = g0.astype(jnp.bfloat16)
        dw2 = jnp.dot(z.T, dY, preferred_element_type=jnp.float32)
        g = jnp.dot(dY, b.T, preferred_element_type=jnp.float32)
        dz = (g * g1).astype(jnp.bfloat16)
        acc = acc + jnp.dot(dz, a.T, preferred_element_type=jnp.float32)
        dw1 = jnp.dot(X.T, dz, preferred_element_type=jnp.float32)
        return acc, (dw1, dw2)

    acc, (dw1, dw2) = lax.scan(step, jnp.zeros((T, H), jnp.float32), (w1c, w2c))
    dX = acc.astype(jnp.bfloat16)
    dW1 = dw1.transpose(1, 0, 2).reshape(H, F)
    dW2 = dw2.reshape(F, H)
    return (dX, dW1, dW2)
```

```python
import math

import jax
import jax.numpy as jnp
from jax import lax
from jax.experimental import pallas as pl
from jax.experimental.pallas import tpu as pltpu
from jax.sharding import PartitionSpec as P

C0 = math.sqrt(2.0 / math.pi)
C1 = 0.044715
BF16 = jnp.bfloat16
F32 = jnp.float32
X, Y = 0, 1
LEFT, RIGHT, PARTNER = 0, 1, 2
MIB = 1 << 20


def _gelu(u):
    t = jnp.tanh(C0 * (u + C1 * u * u * u))
    return 0.5 * u * (1.0 + t), 0.5 * (1.0 + t) + 0.5 * u * (1.0 - t * t) * C0 * (1.0 + 3.0 * C1 * u * u)


def _slot_of(z, q):
    qm = jnp.where(z < 2, q, 3 - q)
    end = jnp.logical_or(z == 0, z == 3)
    return jnp.where(jnp.logical_or(end, qm == 3), qm, (qm + 2) % 3)


def _chip_at(z, k):
    end = jnp.logical_or(z == 0, z == 3)
    qm = k if k == 3 else jnp.where(end, k, (k + 1) % 3)
    return jnp.where(z < 2, qm, 3 - qm)


def _gather_kernel(rows, x_hbm, y_hbm, w1_hbm, w2_hbm,
                   xo, yo, zo, dzo, dx_ref,
                   xg, yg, zs, dzs, g1s, w1, w2, w1t, w2t, pdx, psend, precv, rsend, rrecv,
                   in_sem, w_sem, out_sem, ag_send, ag_recv, ag_precv,
                   p_send, p_recv, r_send, r_recv):
    t = lax.axis_index('tp')
    z, c = t // 2, t % 2
    chunk = 2 * rows
    f, h = w2.shape
    has_left, has_right = z > 0, z < 3
    bufs = (xg, yg)

    def dev(chip, core):
        return {'tp': 2 * chip + core}

    def block(a, slot, core):
        return bufs[a].at[pl.ds(pl.multiple_of(slot * chunk + core * rows, rows), rows), :]

    loads = [pltpu.make_async_copy(src, block(a, 0, c), in_sem.at[a]) for a, src in ((X, x_hbm), (Y, y_hbm))]
    wloads = [pltpu.make_async_copy(src, dst, w_sem.at[i]) for i, (src, dst) in enumerate(((w2_hbm, w2), (w1_hbm, w1)))]
    for cp in loads + wloads:
        cp.start()

    barrier = pltpu.get_barrier_semaphore()
    pl.semaphore_signal(barrier, inc=1, device_id=dev(z, 1 - c), device_id_type=pl.DeviceIdType.MESH)

    @pl.when(has_left)
    def _():
        pl.semaphore_signal(barrier, inc=1, device_id=dev(z - 1, c), device_id_type=pl.DeviceIdType.MESH)

    @pl.when(has_right)
    def _():
        pl.semaphore_signal(barrier, inc=1, device_id=dev(z + 1, c), device_id_type=pl.DeviceIdType.MESH)

    @pl.when(jnp.logical_and(has_left, has_right))
    def _():
        pl.semaphore_wait(barrier, 3)

    @pl.when(jnp.logical_not(jnp.logical_and(has_left, has_right)))
    def _():
        pl.semaphore_wait(barrier, 2)

    def ag_copy(a, q, to):
        chip = {LEFT: z - 1, RIGHT: z + 1, PARTNER: z}[to]
        core = 1 - c if to == PARTNER else c
        recv = ag_precv if to == PARTNER else ag_recv
        return pltpu.make_async_remote_copy(
            src_ref=block(a, _slot_of(z, q), c), dst_ref=block(a, _slot_of(chip, q), c),
            send_sem=ag_send.at[to, a, q], recv_sem=recv.at[a, q],
            device_id=dev(chip, core), device_id_type=pl.DeviceIdType.MESH)

    def ag_forward(a, q, to):
        ok = {LEFT: has_left, RIGHT: has_right}[to]

        @pl.when(ok)
        def _():
            ag_copy(a, q, to).start()

    def ag_wait(a, q, core, recv):
        dst = block(a, _slot_of(z, q), core)
        pltpu.make_async_copy(dst, dst, recv.at[a, q]).wait()

    for a in (X, Y):
        loads[a].wait()
        ag_forward(a, z, RIGHT)
        ag_forward(a, z, LEFT)
        ag_copy(a, z, PARTNER).start()

    def arrivals(a, d):
        @pl.when(z - d >= 0)
        def _():
            ag_wait(a, z - d, c, ag_recv)
            ag_forward(a, z - d, RIGHT)
            ag_copy(a, z - d, PARTNER).start()

        @pl.when(z + d <= 3)
        def _():
            ag_wait(a, z + d, c, ag_recv)
            ag_forward(a, z + d, LEFT)
            ag_copy(a, z + d, PARTNER).start()

    def partner_wait(a, k):
        ag_wait(a, _chip_at(z, k), 1 - c, ag_precv)

    wloads[0].wait()

    @pl.loop(0, f // 256)
    def _(i):
        s = pl.ds(pl.multiple_of(i * 256, 256), 256)
        w2t[:, s] = w2[s, :].T

    wloads[1].wait()

    @pl.loop(0, h // 256)
    def _(i):
        s = pl.ds(pl.multiple_of(i * 256, 256), 256)
        w1t[:, s] = w1[s, :].T

    def step_u(r0, m):
        r = pl.ds(r0, m)

        @pl.loop(0, f // 512)
        def _(n):
            s = pl.ds(pl.multiple_of(n * 512, 512), 512)
            u = jnp.dot(xg[r, :], w1[:, s], preferred_element_type=F32).astype(BF16)
            g0, g1 = _gelu(u.astype(F32))
            zs[r, s] = g0.astype(BF16)
            g1s[r, s] = g1

    def step_g(r0, m):
        r = pl.ds(r0, m)

        @pl.loop(0, f // 512)
        def _(n):
            s = pl.ds(pl.multiple_of(n * 512, 512), 512)
            g = jnp.dot(yg[r, :], w2t[:, s], preferred_element_type=F32)
            dzs[r, s] = (g * g1s[r, s]).astype(BF16)

    def step_dx(r0, m):
        r = pl.ds(r0, m)

        @pl.loop(0, h // 512)
        def _(n):
            s = pl.ds(pl.multiple_of(n * 512, 512), 512)
            pdx[r, s] = jnp.dot(dzs[r, :], w1t[:, s], preferred_element_type=F32)

    def pair_copy(k):
        return pltpu.make_async_remote_copy(
            src_ref=psend.at[k], dst_ref=precv.at[k], send_sem=p_send.at[k], recv_sem=p_recv.at[k],
            device_id=dev(z, 1 - c), device_id_type=pl.DeviceIdType.MESH)

    def rs_copy(k):
        q = _chip_at(z, k)
        s = _slot_of(q, z)
        return pltpu.make_async_remote_copy(
            src_ref=rsend.at[k], dst_ref=rrecv.at[s], send_sem=r_send.at[k], recv_sem=r_recv.at[s],
            device_id=dev(q, c), device_id_type=pl.DeviceIdType.MESH)

    def part(k, core):
        return pdx[pl.ds(pl.multiple_of(k * chunk + core * rows, rows), rows), :]

    def pair_start(k):
        psend[k] = part(k, 1 - c).astype(BF16)
        pair_copy(k).start()

    def rs_start(k):
        pair_copy(k).wait_recv()
        rsend[k] = (part(k, c) + precv[k].astype(F32)).astype(BF16)
        rs_copy(k).start()

    arrivals(X, 1)
    partner_wait(X, 0)
    step_u(0, chunk)
    partner_wait(Y, 0)
    step_g(0, chunk)
    arrivals(Y, 1)
    step_dx(0, chunk)
    pair_start(0)
    arrivals(X, 2)
    partner_wait(X, 1)
    partner_wait(X, 2)
    step_u(chunk, 2 * chunk)
    arrivals(Y, 2)
    partner_wait(Y, 1)
    partner_wait(Y, 2)
    step_g(chunk, 2 * chunk)
    step_dx(chunk, 2 * chunk)
    pair_start(1)
    pair_start(2)
    rs_start(1)
    rs_start(2)
    arrivals(X, 3)
    partner_wait(X, 3)
    xout = pltpu.make_async_copy(xg, xo, out_sem.at[0])
    xout.start()
    step_u(3 * chunk, chunk)
    zout = pltpu.make_async_copy(zs, zo, out_sem.at[1])
    zout.start()
    arrivals(Y, 3)
    partner_wait(Y, 3)
    yout = pltpu.make_async_copy(yg, yo, out_sem.at[2])
    yout.start()
    step_g(3 * chunk, chunk)
    dzout = pltpu.make_async_copy(dzs, dzo, out_sem.at[3])
    dzout.start()
    step_dx(3 * chunk, chunk)
    pair_start(3)
    rs_start(3)

    pair_copy(0).wait_recv()
    total = part(0, c) + precv[0].astype(F32)
    for k in (1, 2, 3):
        pltpu.make_async_copy(rrecv.at[k], rrecv.at[k], r_recv.at[k]).wait()
        total += rrecv[k].astype(F32)
    dx_ref[...] = total.astype(BF16)

    def ag_drain(a, q, to):
        ok = {LEFT: has_left, RIGHT: has_right}[to]

        @pl.when(ok)
        def _():
            ag_copy(a, q, to).wait_send()

    for a in (X, Y):
        ag_drain(a, z, RIGHT)
        ag_drain(a, z, LEFT)
        ag_copy(a, z, PARTNER).wait_send()
        for d in (1, 2, 3):
            @pl.when(z - d >= 0)
            def _():
                ag_drain(a, z - d, RIGHT)
                ag_copy(a, z - d, PARTNER).wait_send()

            @pl.when(z + d <= 3)
            def _():
                ag_drain(a, z + d, LEFT)
                ag_copy(a, z + d, PARTNER).wait_send()
    for k in range(4):
        pair_copy(k).wait_send()
    for k in (1, 2, 3):
        rs_copy(k).wait_send()
    for cp in (xout, yout, zout, dzout):
        cp.wait()


def _dw_kernel(xb, dz, zb, y, dxi, dw1, dw2, dx):
    dims = (((0,), (0,)), ((), ()))
    dw1[...] = lax.dot_general(xb[...], dz[...], dims, preferred_element_type=F32)
    dw2[...] = lax.dot_general(zb[...], y[...], dims, preferred_element_type=F32)

    @pl.when(pl.program_id(0) == 0)
    def _():
        dx[...] = dxi[...]


def solution(mesh):
    def body(x, dy, w1, w2):
        rows, h = x.shape
        f = w1.shape[1]
        n = 8 * rows
        vm = pltpu.VMEM
        sem = pltpu.SemaphoreType.DMA
        anyspec = pl.BlockSpec(memory_space=pl.ANY)
        xg, yg, zg, dzg, dx = pl.pallas_call(
            lambda *refs: _gather_kernel(rows, *refs),
            out_shape=(
                jax.ShapeDtypeStruct((n, h), BF16), jax.ShapeDtypeStruct((n, h), BF16),
                jax.ShapeDtypeStruct((n, f), BF16), jax.ShapeDtypeStruct((n, f), BF16),
                jax.ShapeDtypeStruct((rows, h), BF16)),
            in_specs=[anyspec] * 4,
            out_specs=(anyspec,) * 4 + (pl.BlockSpec(memory_space=pltpu.VMEM),),
            scratch_shapes=[
                vm((n, h), BF16), vm((n, h), BF16), vm((n, f), BF16), vm((n, f), BF16), vm((n, f), F32),
                vm((h, f), BF16), vm((f, h), BF16), vm((f, h), BF16), vm((h, f), BF16),
                vm((n, h), F32), vm((4, rows, h), BF16), vm((4, rows, h), BF16),
                vm((4, rows, h), BF16), vm((4, rows, h), BF16),
                sem((2,)), sem((2,)), sem((4,)), sem((3, 2, 4)), sem((2, 4)), sem((2, 4)),
                sem((4,)), sem((4,)), sem((4,)), sem((4,)),
            ],
            compiler_params=pltpu.CompilerParams(
                collective_id=0, has_side_effects=True, vmem_limit_bytes=56 * MIB),
            name='gather_dx',
        )(x, dy, w1, w2)
        steps = 8
        hb, fb = h // steps, f // steps
        dw1, dw2, dx = pl.pallas_call(
            _dw_kernel,
            grid=(steps,),
            out_shape=(jax.ShapeDtypeStruct((h, f), F32), jax.ShapeDtypeStruct((f, h), F32),
                       jax.ShapeDtypeStruct((rows, h), BF16)),
            in_specs=[
                pl.BlockSpec((n, hb), lambda i: (0, i)), pl.BlockSpec((n, f), lambda i: (0, 0)),
                pl.BlockSpec((n, fb), lambda i: (0, i)), pl.BlockSpec((n, h), lambda i: (0, 0)),
                pl.BlockSpec((rows, h), lambda i: (0, 0)),
            ],
            out_specs=(
                pl.BlockSpec((hb, f), lambda i: (i, 0)), pl.BlockSpec((fb, h), lambda i: (i, 0)),
                pl.BlockSpec((rows, h), lambda i: (0, 0)),
            ),
            compiler_params=pltpu.CompilerParams(vmem_limit_bytes=40 * MIB),
            name='dw',
        )(xg, dzg, zg, yg, dx)
        return dx, dw1, dw2

    return jax.shard_map(
        body, mesh=mesh,
        in_specs=(P(('dp', 'tp'), None), P(('dp', 'tp'), None), P(None, 'tp'), P('tp', None)),
        out_specs=(P(('dp', 'tp'), None), P('dp', 'tp'), P(('dp', 'tp'), None)),
        check_vma=False)
```

```python
import math

import jax
import jax.numpy as jnp
from jax import lax
from jax.experimental import pallas as pl
from jax.experimental.pallas import tpu as pltpu
from jax.sharding import PartitionSpec as P

C0 = math.sqrt(2.0 / math.pi)
C1 = 0.044715
BF16 = jnp.bfloat16
F32 = jnp.float32
X, Y = 0, 1
LEFT, RIGHT, PARTNER = 0, 1, 2
MIB = 1 << 20


def _gelu(u):
    t = jnp.tanh(C0 * (u + C1 * u * u * u))
    return 0.5 * u * (1.0 + t), 0.5 * (1.0 + t) + 0.5 * u * (1.0 - t * t) * C0 * (1.0 + 3.0 * C1 * u * u)


def _slot_of(z, q):
    qm = jnp.where(z < 2, q, 3 - q)
    end = jnp.logical_or(z == 0, z == 3)
    return jnp.where(jnp.logical_or(end, qm == 3), qm, (qm + 2) % 3)


def _chip_at(z, k):
    end = jnp.logical_or(z == 0, z == 3)
    qm = k if k == 3 else jnp.where(end, k, (k + 1) % 3)
    return jnp.where(z < 2, qm, 3 - qm)


def _gather_kernel(rows, x_hbm, y_hbm, w1_hbm, w2_hbm,
                   xg, yg, zs, dzs, dx_ref,
                   g1s, w1, w2, w1t, w2t, pdx, psend, precv, rsend, rrecv,
                   in_sem, w_sem, ag_send, ag_recv, ag_precv,
                   p_send, p_recv, r_send, r_recv):
    t = lax.axis_index('tp')
    z, c = t // 2, t % 2
    chunk = 2 * rows
    f, h = w2.shape
    has_left, has_right = z > 0, z < 3
    bufs = (xg, yg)

    def dev(chip, core):
        return {'tp': 2 * chip + core}

    def block(a, slot, core):
        return bufs[a].at[pl.ds(pl.multiple_of(slot * chunk + core * rows, rows), rows), :]

    loads = [pltpu.make_async_copy(src, block(a, 0, c), in_sem.at[a]) for a, src in ((X, x_hbm), (Y, y_hbm))]
    wloads = [pltpu.make_async_copy(src, dst, w_sem.at[i]) for i, (src, dst) in enumerate(((w2_hbm, w2), (w1_hbm, w1)))]
    for cp in loads + wloads:
        cp.start()

    barrier = pltpu.get_barrier_semaphore()
    pl.semaphore_signal(barrier, inc=1, device_id=dev(z, 1 - c), device_id_type=pl.DeviceIdType.MESH)

    @pl.when(has_left)
    def _():
        pl.semaphore_signal(barrier, inc=1, device_id=dev(z - 1, c), device_id_type=pl.DeviceIdType.MESH)

    @pl.when(has_right)
    def _():
        pl.semaphore_signal(barrier, inc=1, device_id=dev(z + 1, c), device_id_type=pl.DeviceIdType.MESH)

    @pl.when(jnp.logical_and(has_left, has_right))
    def _():
        pl.semaphore_wait(barrier, 3)

    @pl.when(jnp.logical_not(jnp.logical_and(has_left, has_right)))
    def _():
        pl.semaphore_wait(barrier, 2)

    def ag_copy(a, q, to):
        chip = {LEFT: z - 1, RIGHT: z + 1, PARTNER: z}[to]
        core = 1 - c if to == PARTNER else c
        recv = ag_precv if to == PARTNER else ag_recv
        return pltpu.make_async_remote_copy(
            src_ref=block(a, _slot_of(z, q), c), dst_ref=block(a, _slot_of(chip, q), c),
            send_sem=ag_send.at[to, a, q], recv_sem=recv.at[a, q],
            device_id=dev(chip, core), device_id_type=pl.DeviceIdType.MESH)

    def ag_forward(a, q, to):
        ok = {LEFT: has_left, RIGHT: has_right}[to]

        @pl.when(ok)
        def _():
            ag_copy(a, q, to).start()

    def ag_wait(a, q, core, recv):
        dst = block(a, _slot_of(z, q), core)
        pltpu.make_async_copy(dst, dst, recv.at[a, q]).wait()

    for a in (X, Y):
        loads[a].wait()
        ag_forward(a, z, RIGHT)
        ag_forward(a, z, LEFT)
        ag_copy(a, z, PARTNER).start()

    def arrivals(a, d):
        @pl.when(z - d >= 0)
        def _():
            ag_wait(a, z - d, c, ag_recv)
            ag_forward(a, z - d, RIGHT)
            ag_copy(a, z - d, PARTNER).start()

        @pl.when(z + d <= 3)
        def _():
            ag_wait(a, z + d, c, ag_recv)
            ag_forward(a, z + d, LEFT)
            ag_copy(a, z + d, PARTNER).start()

    def partner_wait(a, k):
        ag_wait(a, _chip_at(z, k), 1 - c, ag_precv)

    wloads[0].wait()

    @pl.loop(0, f // 256)
    def _(i):
        s = pl.ds(pl.multiple_of(i * 256, 256), 256)
        w2t[:, s] = w2[s, :].T

    wloads[1].wait()

    @pl.loop(0, h // 256)
    def _(i):
        s = pl.ds(pl.multiple_of(i * 256, 256), 256)
        w1t[:, s] = w1[s, :].T

    def step_u(r0, m):
        r = pl.ds(r0, m)

        @pl.loop(0, f // 512)
        def _(n):
            s = pl.ds(pl.multiple_of(n * 512, 512), 512)
            u = jnp.dot(xg[r, :], w1[:, s], preferred_element_type=F32).astype(BF16)
            g0, g1 = _gelu(u.astype(F32))
            zs[r, s] = g0.astype(BF16)
            g1s[r, s] = g1

    def step_g(r0, m):
        r = pl.ds(r0, m)

        @pl.loop(0, f // 512)
        def _(n):
            s = pl.ds(pl.multiple_of(n * 512, 512), 512)
            g = jnp.dot(yg[r, :], w2t[:, s], preferred_element_type=F32)
            dzs[r, s] = (g * g1s[r, s]).astype(BF16)

    def step_dx(r0, m):
        r = pl.ds(r0, m)

        @pl.loop(0, h // 512)
        def _(n):
            s = pl.ds(pl.multiple_of(n * 512, 512), 512)
            pdx[r, s] = jnp.dot(dzs[r, :], w1t[:, s], preferred_element_type=F32)

    def pair_copy(k):
        return pltpu.make_async_remote_copy(
            src_ref=psend.at[k], dst_ref=precv.at[k], send_sem=p_send.at[k], recv_sem=p_recv.at[k],
            device_id=dev(z, 1 - c), device_id_type=pl.DeviceIdType.MESH)

    def rs_copy(k):
        q = _chip_at(z, k)
        s = _slot_of(q, z)
        return pltpu.make_async_remote_copy(
            src_ref=rsend.at[k], dst_ref=rrecv.at[s], send_sem=r_send.at[k], recv_sem=r_recv.at[s],
            device_id=dev(q, c), device_id_type=pl.DeviceIdType.MESH)

    def part(k, core):
        return pdx[pl.ds(pl.multiple_of(k * chunk + core * rows, rows), rows), :]

    def pair_start(k):
        psend[k] = part(k, 1 - c).astype(BF16)
        pair_copy(k).start()

    def rs_start(k):
        pair_copy(k).wait_recv()
        rsend[k] = (part(k, c) + precv[k].astype(F32)).astype(BF16)
        rs_copy(k).start()

    arrivals(X, 1)
    partner_wait(X, 0)
    step_u(0, chunk)
    partner_wait(Y, 0)
    step_g(0, chunk)
    arrivals(Y, 1)
    step_dx(0, chunk)
    pair_start(0)
    arrivals(X, 2)
    partner_wait(X, 1)
    partner_wait(X, 2)
    step_u(chunk, 2 * chunk)
    arrivals(Y, 2)
    partner_wait(Y, 1)
    partner_wait(Y, 2)
    step_g(chunk, 2 * chunk)
    step_dx(chunk, 2 * chunk)
    pair_start(1)
    pair_start(2)
    rs_start(1)
    rs_start(2)
    arrivals(X, 3)
    partner_wait(X, 3)
    step_u(3 * chunk, chunk)
    arrivals(Y, 3)
    partner_wait(Y, 3)
    step_g(3 * chunk, chunk)
    step_dx(3 * chunk, chunk)
    pair_start(3)
    rs_start(3)

    pair_copy(0).wait_recv()
    total = part(0, c) + precv[0].astype(F32)
    for k in (1, 2, 3):
        pltpu.make_async_copy(rrecv.at[k], rrecv.at[k], r_recv.at[k]).wait()
        total += rrecv[k].astype(F32)
    dx_ref[...] = total.astype(BF16)

    def ag_drain(a, q, to):
        ok = {LEFT: has_left, RIGHT: has_right}[to]

        @pl.when(ok)
        def _():
            ag_copy(a, q, to).wait_send()

    for a in (X, Y):
        ag_drain(a, z, RIGHT)
        ag_drain(a, z, LEFT)
        ag_copy(a, z, PARTNER).wait_send()
        for d in (1, 2, 3):
            @pl.when(z - d >= 0)
            def _():
                ag_drain(a, z - d, RIGHT)
                ag_copy(a, z - d, PARTNER).wait_send()

            @pl.when(z + d <= 3)
            def _():
                ag_drain(a, z + d, LEFT)
                ag_copy(a, z + d, PARTNER).wait_send()
    for k in range(4):
        pair_copy(k).wait_send()
    for k in (1, 2, 3):
        rs_copy(k).wait_send()


def _dw_kernel(xb, dz, zb, y, dxi, dw1, dw2, dx):
    dims = (((0,), (0,)), ((), ()))
    dw1[...] = lax.dot_general(xb[...], dz[...], dims, preferred_element_type=F32)
    dw2[...] = lax.dot_general(zb[...], y[...], dims, preferred_element_type=F32)

    @pl.when(pl.program_id(0) == 0)
    def _():
        dx[...] = dxi[...]


def solution(mesh):
    def body(x, dy, w1, w2):
        rows, h = x.shape
        f = w1.shape[1]
        n = 8 * rows
        vm = pltpu.VMEM
        sem = pltpu.SemaphoreType.DMA
        vspec = pl.BlockSpec(memory_space=vm)
        hbm = pl.BlockSpec(memory_space=pltpu.HBM)
        xg, yg, zg, dzg, dx = pl.pallas_call(
            lambda *refs: _gather_kernel(rows, *refs),
            out_shape=(vm((n, h), BF16), vm((n, h), BF16), vm((n, f), BF16), vm((n, f), BF16), vm((rows, h), BF16)),
            in_specs=[hbm] * 4,
            out_specs=(vspec,) * 5,
            scratch_shapes=[
                vm((n, f), F32),
                vm((h, f), BF16), vm((f, h), BF16), vm((f, h), BF16), vm((h, f), BF16),
                vm((n, h), F32), vm((4, rows, h), BF16), vm((4, rows, h), BF16),
                vm((4, rows, h), BF16), vm((4, rows, h), BF16),
                sem((2,)), sem((2,)), sem((3, 2, 4)), sem((2, 4)), sem((2, 4)),
                sem((4,)), sem((4,)), sem((4,)), sem((4,)),
            ],
            compiler_params=pltpu.CompilerParams(
                collective_id=0, has_side_effects=True, vmem_limit_bytes=40 * MIB),
            name='gather_dx',
        )(*(pltpu.with_memory_space_constraint(a, pltpu.HBM) for a in (x, dy, w1, w2)))
        steps = 8
        hb, fb = h // steps, f // steps
        dw1, dw2, dx = pl.pallas_call(
            _dw_kernel,
            grid=(steps,),
            out_shape=(jax.ShapeDtypeStruct((h, f), F32), jax.ShapeDtypeStruct((f, h), F32),
                       jax.ShapeDtypeStruct((rows, h), BF16)),
            in_specs=[
                pl.BlockSpec((n, hb), lambda i: (0, i)), pl.BlockSpec((n, f), lambda i: (0, 0)),
                pl.BlockSpec((n, fb), lambda i: (0, i)), pl.BlockSpec((n, h), lambda i: (0, 0)),
                pl.BlockSpec((rows, h), lambda i: (0, 0)),
            ],
            out_specs=(
                pl.BlockSpec((hb, f), lambda i: (i, 0)), pl.BlockSpec((fb, h), lambda i: (i, 0)),
                pl.BlockSpec((rows, h), lambda i: (0, 0)),
            ),
            compiler_params=pltpu.CompilerParams(vmem_limit_bytes=40 * MIB),
            name='dw',
        )(xg, dzg, zg, yg, dx)
        return dx, dw1, dw2

    return jax.shard_map(
        body, mesh=mesh,
        in_specs=(P(('dp', 'tp'), None), P(('dp', 'tp'), None), P(None, 'tp'), P('tp', None)),
        out_specs=(P(('dp', 'tp'), None), P('dp', 'tp'), P(('dp', 'tp'), None)),
        check_vma=False)
```

```python
import math

import jax
import jax.numpy as jnp
from jax import lax
from jax.experimental import pallas as pl
from jax.experimental.pallas import tpu as pltpu
from jax.sharding import PartitionSpec as P


C0 = math.sqrt(2.0 / math.pi)
C1 = 0.044715
BF16 = jnp.bfloat16
F32 = jnp.float32
X, Y = 0, 1
MESH = pl.DeviceIdType.MESH
MIB = 1 << 20


def _gelu(u):
    t = jnp.tanh(C0 * (u + C1 * u * u * u))
    return 0.5 * u * (1.0 + t), 0.5 * (1.0 + t) + 0.5 * u * (1.0 - t * t) * C0 * (1.0 + 3.0 * C1 * u * u)


def _gather_kernel(rows, x_hbm, y_hbm, w1_hbm, w2_hbm,
                   xg, yg, zs, dzs, acc_ref, last_ref, mid_ref,
                   g1s, w1, w2, w1t, w2t, pdx, psend, precv, rsend, rrecv,
                   in_sem, w_sem, ag_send, ag_psend, ag_recv, ag_precv,
                   p_send, p_recv, r_send, r_recv):
    t = lax.axis_index('tp')
    z, c = t // 2, t % 2
    chunk = 2 * rows
    f, h = w2.shape
    low = z < 2
    near_end, near_mid = jnp.where(low, 0, 3), jnp.where(low, 1, 2)
    far_mid, far_end = 3 - near_mid, 3 - near_end
    is_end = z == near_end
    is_mid = jnp.logical_not(is_end)
    bufs = (xg, yg)

    def dev(chip, core):
        return {'tp': 2 * chip + core}

    def block(a, slot, core):
        return bufs[a].at[pl.ds(pl.multiple_of(slot * chunk + core * rows, rows), rows), :]

    loads = [pltpu.make_async_copy(src, block(a, 0, c), in_sem.at[a]) for a, src in ((X, x_hbm), (Y, y_hbm))]
    piece = 256
    w2loads = [(w2_hbm, w2, i) for i in range(f // piece)]
    w1loads = [(w1_hbm, w1, i) for i in range(h // piece)]

    def wload(src, dst, i, j):
        s = pl.ds(i * piece, piece)
        return pltpu.make_async_copy(src.at[s, :], dst.at[s, :], w_sem.at[j])

    wloads = [wload(*x, j) for j, x in enumerate(w2loads + w1loads)]
    for cp in loads:
        cp.start()

    barrier = pltpu.get_barrier_semaphore()

    def greet(chip, core):
        pl.semaphore_signal(barrier, inc=1, device_id=dev(chip, core), device_id_type=MESH)

    greet(z, 1 - c)

    @pl.when(is_end)
    def _():
        greet(near_mid, c)

    @pl.when(is_mid)
    def _():
        greet(near_end, c)
        greet(far_mid, c)
        greet(far_end, c)

    for cp in loads:
        cp.wait()
    for cp in wloads:
        cp.start()
    pl.semaphore_wait(barrier, 3)

    def ag_copy(a, i, slot, chip, to_slot):
        return pltpu.make_async_remote_copy(
            src_ref=block(a, slot, c), dst_ref=block(a, to_slot, c),
            send_sem=ag_send.at[a, i], recv_sem=ag_recv.at[a, to_slot],
            device_id=dev(chip, c), device_id_type=MESH)

    def share(a, slot):
        return pltpu.make_async_remote_copy(
            src_ref=block(a, slot, c), dst_ref=block(a, slot, c),
            send_sem=ag_psend.at[a, slot], recv_sem=ag_precv.at[a, slot],
            device_id=dev(z, 1 - c), device_id_type=MESH)

    def end_msg(a, i):
        return ag_copy(a, i, 0, *((far_mid, 1), (near_mid, 3))[i])

    def mid_msg(a, i):
        return ag_copy(a, i, *((0, near_end, 1), (0, far_mid, 2), (1, near_end, 2), (2, near_end, 3))[i])

    def arrive(a, slot, forward=None):
        dst = block(a, slot, c)
        pltpu.make_async_copy(dst, dst, ag_recv.at[a, slot]).wait()
        if forward is not None:
            mid_msg(a, forward).start()
        share(a, slot).start()

    def partner(a, slot):
        share(a, slot).wait_recv()

    def step_u(slot, m=1):
        r = pl.ds(slot * chunk, m * chunk)

        @pl.loop(0, f // 512)
        def _(n):
            s = pl.ds(pl.multiple_of(n * 512, 512), 512)
            u = jnp.dot(xg[r, :], w1[:, s], preferred_element_type=F32).astype(BF16)
            g0, g1 = _gelu(u.astype(F32))
            zs[r, s] = g0.astype(BF16)
            g1s[r, s] = g1

    def step_g(slot, m=1):
        r = pl.ds(slot * chunk, m * chunk)

        @pl.loop(0, f // 512)
        def _(n):
            s = pl.ds(pl.multiple_of(n * 512, 512), 512)
            g = jnp.dot(yg[r, :], w2t[:, s], preferred_element_type=F32)
            dzs[r, s] = (g * g1s[r, s]).astype(BF16)

    def step_dx(slot, m=1):
        r = pl.ds(slot * chunk, m * chunk)

        @pl.loop(0, h // 512)
        def _(n):
            s = pl.ds(pl.multiple_of(n * 512, 512), 512)
            pdx[r, s] = jnp.dot(dzs[r, :], w1t[:, s], preferred_element_type=F32)

        for k in range(slot, slot + m):
            psend[k] = part(k, 1 - c).astype(BF16)
            pair_copy(k).start()

    def part(k, core):
        return pdx[pl.ds(pl.multiple_of(k * chunk + core * rows, rows), rows), :]

    def pair_copy(k):
        return pltpu.make_async_remote_copy(
            src_ref=psend.at[k], dst_ref=precv.at[k], send_sem=p_send.at[k], recv_sem=p_recv.at[k],
            device_id=dev(z, 1 - c), device_id_type=MESH)

    def pair_sum(k):
        pair_copy(k).wait_recv()
        return part(k, c) + precv[k].astype(F32)

    def rs_copy(k, chip, i):
        return pltpu.make_async_remote_copy(
            src_ref=rsend.at[k], dst_ref=rrecv.at[i], send_sem=r_send.at[k], recv_sem=r_recv.at[i],
            device_id=dev(chip, c), device_id_type=MESH)

    def rs_recv(i):
        pltpu.make_async_copy(rrecv.at[i], rrecv.at[i], r_recv.at[i]).wait()
        return rrecv[i].astype(F32)

    @pl.when(is_end)
    def _():
        end_msg(X, 0).start()

    @pl.when(is_mid)
    def _():
        mid_msg(X, 0).start()

    share(X, 0).start()
    share(Y, 0).start()

    for i in range(f // piece):
        wloads[i].wait()
        w2t[:, i * piece:(i + 1) * piece] = w2[i * piece:(i + 1) * piece, :].T

    @pl.when(is_end)
    def _():
        end_msg(Y, 0).start()

    @pl.when(is_mid)
    def _():
        mid_msg(Y, 0).start()

    for i in range(h // piece):
        wloads[f // piece + i].wait()
        w1t[:, i * piece:(i + 1) * piece] = w1[i * piece:(i + 1) * piece, :].T

    @pl.when(is_end)
    def _():
        partner(X, 0)
        arrive(X, 1)
        end_msg(X, 1).start()
        partner(X, 1)
        step_u(0, 2)
        end_msg(Y, 1).start()
        arrive(Y, 1)
        partner(Y, 0)
        partner(Y, 1)
        step_g(0, 2)
        step_dx(0, 2)
        arrive(X, 2)
        partner(X, 2)
        step_u(2)
        arrive(Y, 2)
        acc_ref[...] = pair_sum(0)
        rsend[1] = pair_sum(1).astype(BF16)
        rs_copy(1, near_mid, 0).start()
        partner(Y, 2)
        step_g(2)
        arrive(X, 3)
        step_dx(2)
        partner(X, 3)
        rsend[2] = pair_sum(2).astype(BF16)
        rs_copy(2, far_end, 0).start()
        step_u(3)
        arrive(Y, 3)
        partner(Y, 3)
        step_g(3)
        step_dx(3)
        last_ref[...] = pair_sum(3).astype(BF16)
        mid_ref[...] = jnp.zeros_like(mid_ref)
        acc_ref[...] += rs_recv(0)
        for a in (X, Y):
            end_msg(a, 0).wait_send()
            end_msg(a, 1).wait_send()
        rs_copy(1, near_mid, 0).wait_send()
        rs_copy(2, far_end, 0).wait_send()

    @pl.when(is_mid)
    def _():
        partner(X, 0)
        arrive(X, 1, forward=2)
        mid_msg(X, 1).start()
        partner(X, 1)
        step_u(0, 2)
        mid_msg(Y, 1).start()
        arrive(Y, 1, forward=2)
        partner(Y, 0)
        partner(Y, 1)
        step_g(0, 2)
        arrive(X, 2, forward=3)
        arrive(X, 3)
        step_dx(0, 2)
        arrive(Y, 2, forward=3)
        partner(X, 2)
        partner(X, 3)
        step_u(2, 2)
        arrive(Y, 3)
        acc_ref[...] = pair_sum(0)
        rsend[1] = pair_sum(1).astype(BF16)
        rs_copy(1, far_mid, 1).start()
        partner(Y, 2)
        partner(Y, 3)
        step_g(2, 2)
        step_dx(2, 2)
        mid_ref[...] = pair_sum(2).astype(BF16)
        last_ref[...] = (pair_sum(3) + rs_recv(1)).astype(BF16)
        acc_ref[...] += rs_recv(0)
        for a in (X, Y):
            for i in range(4):
                mid_msg(a, i).wait_send()
        rs_copy(1, far_mid, 1).wait_send()

    for a in (X, Y):
        for k in range(4):
            share(a, k).wait_send()
    for k in range(4):
        pair_copy(k).wait_send()


def _dw_kernel(x, dz, zz, y, dw1, dw2, b1, b2, sem):
    dims = (((0,), (0,)), ((), ()))
    n = sem.shape[1]
    hb, fb = x.shape[1] // n, zz.shape[1] // n

    def out(j, i):
        src, dst, m = ((b1, dw1, hb), (b2, dw2, fb))[j]
        s = pl.ds(i * m, m)
        return pltpu.make_async_copy(src.at[s, :], dst.at[s, :], sem.at[j, i])

    for i in range(n):
        b1[pl.ds(i * hb, hb), :] = lax.dot_general(
            x[:, pl.ds(i * hb, hb)], dz[...], dims, preferred_element_type=F32)
        out(0, i).start()
        b2[pl.ds(i * fb, fb), :] = lax.dot_general(
            zz[:, pl.ds(i * fb, fb)], y[...], dims, preferred_element_type=F32)
        out(1, i).start()
    for i in range(n):
        out(0, i).wait()
        out(1, i).wait()


def solution(mesh):
    def body(x, dy, w1, w2):
        rows, h = x.shape
        f = w1.shape[1]
        n = 8 * rows
        vm = pltpu.VMEM
        sem = pltpu.SemaphoreType.DMA
        vspec = pl.BlockSpec(memory_space=vm)
        hbm = pl.BlockSpec(memory_space=pltpu.HBM)
        xg, yg, zg, dzg, acc, last, mid = pl.pallas_call(
            lambda *refs: _gather_kernel(rows, *refs),
            out_shape=(vm((n, h), BF16), vm((n, h), BF16), vm((n, f), BF16), vm((n, f), BF16),
                       vm((rows, h), F32), vm((rows, h), BF16), vm((rows, h), BF16)),
            in_specs=[hbm] * 4,
            out_specs=(vspec,) * 7,
            scratch_shapes=[
                vm((n, f), F32),
                vm((h, f), BF16), vm((f, h), BF16), vm((f, h), BF16), vm((h, f), BF16),
                vm((n, h), F32), vm((4, rows, h), BF16), vm((4, rows, h), BF16),
                vm((3, rows, h), BF16), vm((2, rows, h), BF16),
                sem((2,)), sem(((f + h) // 256,)), sem((2, 4)), sem((2, 4)), sem((2, 4)), sem((2, 4)),
                sem((4,)), sem((4,)), sem((3,)), sem((2,)),
            ],
            compiler_params=pltpu.CompilerParams(
                collective_id=0, has_side_effects=True, vmem_limit_bytes=40 * MIB),
            name='gather_dx',
        )(*(pltpu.with_memory_space_constraint(a, pltpu.HBM) for a in (x, dy, w1, w2)))
        mid = lax.ppermute(mid, 'tp', [(2, 4), (3, 5), (4, 2), (5, 3)])
        hops = ((0, 2), (2, 3), (3, 1), (1, 0))
        far = lax.ppermute(last, 'tp', [(2 * a + c, 2 * b + c) for a, b in hops for c in (0, 1)])
        steps = 8
        dw1, dw2 = pl.pallas_call(
            _dw_kernel,
            out_shape=(jax.ShapeDtypeStruct((h, f), F32), jax.ShapeDtypeStruct((f, h), F32)),
            in_specs=[vspec] * 4,
            out_specs=(hbm,) * 2,
            scratch_shapes=[vm((h, f), F32), vm((f, h), F32), sem((2, steps))],
            compiler_params=pltpu.CompilerParams(vmem_limit_bytes=24 * MIB),
            cost_estimate=pl.CostEstimate(
                flops=4 * n * h * f, bytes_accessed=8 * h * f, transcendentals=0),
            name='dw',
        )(xg, dzg, zg, yg)
        dx = (acc + far.astype(F32) + mid.astype(F32)).astype(BF16)
        return dx, dw1, dw2

    return jax.shard_map(
        body, mesh=mesh,
        in_specs=(P(('dp', 'tp'), None), P(('dp', 'tp'), None), P(None, 'tp'), P('tp', None)),
        out_specs=(P(('dp', 'tp'), None), P('dp', 'tp'), P(('dp', 'tp'), None)),
        check_vma=False)
```

```python
import math

import jax
import jax.numpy as jnp
from jax import lax
from jax.experimental import pallas as pl
from jax.experimental.pallas import tpu as pltpu
from jax.sharding import PartitionSpec as P


C0 = math.sqrt(2.0 / math.pi)
C1 = 0.044715
BF16 = jnp.bfloat16
F32 = jnp.float32
X, Y, Y0, Y1 = range(4)
MESH = pl.DeviceIdType.MESH
MIB = 1 << 20


def _gelu(u):
    t = jnp.tanh(C0 * (u + C1 * u * u * u))
    return 0.5 * u * (1.0 + t), 0.5 * (1.0 + t) + 0.5 * u * (1.0 - t * t) * C0 * (1.0 + 3.0 * C1 * u * u)


def _gather_kernel(rows, x_hbm, y_hbm, w1_hbm, w2_hbm,
                   xg, yg, zs, dzs, acc_ref, last_ref, mid_ref,
                   g1s, w1, w2, w1t, w2t, pdx, psend, precv, rsend, rrecv,
                   in_sem, w_sem, ag_send, ag_recv, ag_precv, p_recv, r_recv):
    t = lax.axis_index('tp')
    z, c = t // 2, t % 2
    chunk = 2 * rows
    f, h = w2.shape
    low = z < 2
    near_end, near_mid = jnp.where(low, 0, 3), jnp.where(low, 1, 2)
    far_mid, far_end = 3 - near_mid, 3 - near_end
    is_end = z == near_end
    is_mid = jnp.logical_not(is_end)

    def dev(chip, core):
        return {'tp': 2 * chip + core}

    def block(a, slot, core):
        r = pl.ds(pl.multiple_of(slot * chunk + core * rows, rows), rows)
        if a in (X, Y):
            return (xg, yg)[a].at[r, :]
        return yg.at[r, pl.ds((a - Y0) * (h // 2), h // 2)]

    def flag(a):
        return {X: 0, Y: 1, Y0: 1, Y1: 2}[a]

    loads = [pltpu.make_async_copy(src, block(a, 0, c), in_sem.at[a]) for a, src in ((X, x_hbm), (Y, y_hbm))]
    piece = 256
    w2loads = [(w2_hbm, w2, i) for i in range(f // piece)]
    w1loads = [(w1_hbm, w1, i) for i in range(h // piece)]

    def wload(src, dst, i, j):
        s = pl.ds(i * piece, piece)
        return pltpu.make_async_copy(src.at[s, :], dst.at[s, :], w_sem.at[j])

    wloads = [wload(*x, j) for j, x in enumerate(w2loads + w1loads)]
    for cp in loads:
        cp.start()

    barrier = pltpu.get_barrier_semaphore()

    def greet(chip, core):
        pl.semaphore_signal(barrier, inc=1, device_id=dev(chip, core), device_id_type=MESH)

    greet(z, 1 - c)

    @pl.when(is_end)
    def _():
        greet(near_mid, c)

    @pl.when(is_mid)
    def _():
        greet(near_end, c)
        greet(far_mid, c)
        greet(far_end, c)

    for cp in loads:
        cp.wait()
    for cp in wloads:
        cp.start()
    pl.semaphore_wait(barrier, 3)

    def ag_copy(a, slot, chip, to_slot):
        return pltpu.make_async_remote_copy(
            src_ref=block(a, slot, c), dst_ref=block(a, to_slot, c),
            send_sem=ag_send, recv_sem=ag_recv.at[flag(a), to_slot],
            device_id=dev(chip, c), device_id_type=MESH)

    def share(a, slot):
        return pltpu.make_async_remote_copy(
            src_ref=block(a, slot, c), dst_ref=block(a, slot, c),
            send_sem=ag_send, recv_sem=ag_precv.at[flag(a), slot],
            device_id=dev(z, 1 - c), device_id_type=MESH)

    def end_msg(a, i):
        return ag_copy(a, 0, *((far_mid, 1), (near_mid, 3))[i])

    def mid_msg(a, i):
        return ag_copy(a, *((0, near_end, 1), (0, far_mid, 2), (1, near_end, 2), (2, near_end, 3))[i])

    def arrive(a, slot, forward=None):
        dst = block(a, slot, c)
        pltpu.make_async_copy(dst, dst, ag_recv.at[flag(a), slot]).wait()
        if forward is not None:
            mid_msg(a, forward).start()
        share(a, slot).start()

    def partner(a, slot):
        share(a, slot).wait_recv()

    def step_u(slot, m=1):
        r = pl.ds(slot * chunk, m * chunk)

        @pl.loop(0, f // 512)
        def _(n):
            s = pl.ds(pl.multiple_of(n * 512, 512), 512)
            u = jnp.dot(xg[r, :], w1[:, s], preferred_element_type=F32).astype(BF16)
            g0, g1 = _gelu(u.astype(F32))
            zs[r, s] = g0.astype(BF16)
            g1s[r, s] = g1

    def step_g(slot, m=1):
        r = pl.ds(slot * chunk, m * chunk)

        @pl.loop(0, f // 512)
        def _(n):
            s = pl.ds(pl.multiple_of(n * 512, 512), 512)
            g = jnp.dot(yg[r, :], w2t[:, s], preferred_element_type=F32)
            dzs[r, s] = (g * g1s[r, s]).astype(BF16)

    def half_g(slot, i):
        r = pl.ds(slot * chunk, chunk)
        kk = pl.ds(i * (h // 2), h // 2)

        @pl.loop(0, f // 512)
        def _(n):
            s = pl.ds(pl.multiple_of(n * 512, 512), 512)
            g = jnp.dot(yg[r, kk], w2t[kk, s], preferred_element_type=F32)
            if i == 0:
                pdx[r, s] = g
            else:
                dzs[r, s] = ((g + pdx[r, s]) * g1s[r, s]).astype(BF16)

    def step_dx(slot, m=1, half=None):
        r = pl.ds(slot * chunk, m * chunk)
        per = h // 512 if half is None else h // 1024

        @pl.loop(0, per)
        def _(n):
            s = pl.ds(pl.multiple_of(((half or 0) * per + n) * 512, 512), 512)
            pdx[r, s] = jnp.dot(dzs[r, :], w1t[:, s], preferred_element_type=F32)
            for k in range(slot, slot + m):
                psend[k, :, s] = part(k, 1 - c, s).astype(BF16)
                pair_copy(k, s, half).start()

    def part(k, core, s=slice(None)):
        return pdx[pl.ds(pl.multiple_of(k * chunk + core * rows, rows), rows), s]

    def cols(half):
        return slice(None) if half is None else pl.ds(half * (h // 2), h // 2)

    def pair_copy(k, s, half=None):
        return pltpu.make_async_remote_copy(
            src_ref=psend.at[k, :, s], dst_ref=precv.at[k, :, s], send_sem=ag_send,
            recv_sem=p_recv.at[4 if half == 1 else k],
            device_id=dev(z, 1 - c), device_id_type=MESH)

    def pair_sum(k, half=None):
        s = cols(half)
        pair_copy(k, s, half).wait_recv()
        return part(k, c, s) + precv[k, :, s].astype(F32)

    def rs_copy(k, chip, i, half=None):
        s = cols(half)
        return pltpu.make_async_remote_copy(
            src_ref=rsend.at[k, :, s], dst_ref=rrecv.at[i, :, s], send_sem=ag_send,
            recv_sem=r_recv.at[2 if half == 1 else i],
            device_id=dev(chip, c), device_id_type=MESH)

    def rs_recv(i, half=None):
        s = cols(half)
        dst = rrecv.at[i, :, s]
        pltpu.make_async_copy(dst, dst, r_recv.at[2 if half == 1 else i]).wait()
        return rrecv[i, :, s].astype(F32)

    def drain(n):
        for r in (xg, yg, xg.at[pl.ds(0, (n + 12 - 16) * rows), :]):
            pltpu.make_async_copy(r, r, ag_send).wait()

    @pl.when(is_end)
    def _():
        end_msg(X, 0).start()

    @pl.when(is_mid)
    def _():
        mid_msg(X, 0).start()

    share(X, 0).start()
    share(Y, 0).start()

    for i in range(f // piece):
        wloads[i].wait()
        w2t[:, i * piece:(i + 1) * piece] = w2[i * piece:(i + 1) * piece, :].T

    @pl.when(is_end)
    def _():
        end_msg(Y, 0).start()

    @pl.when(is_mid)
    def _():
        mid_msg(Y, 0).start()

    for i in range(h // piece):
        wloads[f // piece + i].wait()
        w1t[:, i * piece:(i + 1) * piece] = w1[i * piece:(i + 1) * piece, :].T

    @pl.when(is_end)
    def _():
        partner(X, 0)
        arrive(X, 1)
        partner(X, 1)
        step_u(0, 2)
        end_msg(X, 1).start()
        arrive(Y, 1)
        partner(Y, 0)
        partner(Y, 1)
        step_g(0, 2)
        end_msg(Y, 1).start()
        step_dx(0, 2)
        arrive(X, 2)
        partner(X, 2)
        step_u(2)
        arrive(Y, 2)
        acc_ref[...] = pair_sum(0)
        rsend[1] = pair_sum(1).astype(BF16)
        rs_copy(1, near_mid, 0).start()
        partner(Y, 2)
        step_g(2)
        for i in (0, 1):
            step_dx(2, half=i)
        arrive(X, 3)
        for i in (0, 1):
            rsend[2, :, cols(i)] = pair_sum(2, i).astype(BF16)
            rs_copy(2, far_end, 0, i).start()
        arrive(Y0, 3)
        partner(X, 3)
        step_u(3)
        arrive(Y1, 3)
        partner(Y0, 3)
        half_g(3, 0)
        partner(Y1, 3)
        half_g(3, 1)
        step_dx(3)
        mid_ref[...] = jnp.zeros_like(mid_ref)
        last_ref[...] = pair_sum(3).astype(BF16)
        for i in (0, 1):
            acc_ref[:, cols(i)] += rs_recv(0, i)
        drain(4 + 2)

    @pl.when(is_mid)
    def _():
        partner(X, 0)
        arrive(X, 1, forward=2)
        partner(X, 1)
        mid_msg(X, 1).start()
        step_u(0, 2)
        mid_msg(Y0, 1).start()
        arrive(Y, 1, forward=2)
        partner(Y, 0)
        partner(Y, 1)
        mid_msg(Y1, 1).start()
        step_g(0, 2)
        step_dx(0, 2)
        arrive(X, 2, forward=3)
        arrive(X, 3)
        arrive(Y0, 2, forward=3)
        acc_ref[...] = pair_sum(0)
        arrive(Y1, 2, forward=3)
        rsend[1] = pair_sum(1).astype(BF16)
        rs_copy(1, far_mid, 1).start()
        partner(X, 2)
        partner(X, 3)
        step_u(2, 2)
        arrive(Y, 3)
        partner(Y0, 2)
        partner(Y1, 2)
        partner(Y, 3)
        step_g(2, 2)
        step_dx(2, 2)
        mid_ref[...] = pair_sum(2).astype(BF16)
        last_ref[...] = (pair_sum(3) + rs_recv(1)).astype(BF16)
        acc_ref[...] += rs_recv(0)
        drain(8 + 1)


def _dw_kernel(x, dz, zz, y, dw1, dw2, b1, b2, sem):
    dims = (((0,), (0,)), ((), ()))
    n = sem.shape[1]
    hb, fb = x.shape[1] // n, zz.shape[1] // n

    def out(j, i):
        src, dst, m = ((b1, dw1, hb), (b2, dw2, fb))[j]
        s = pl.ds(i * m, m)
        return pltpu.make_async_copy(src.at[s, :], dst.at[s, :], sem.at[j, i])

    for i in range(n):
        b1[pl.ds(i * hb, hb), :] = lax.dot_general(
            x[:, pl.ds(i * hb, hb)], dz[...], dims, preferred_element_type=F32)
        out(0, i).start()
        b2[pl.ds(i * fb, fb), :] = lax.dot_general(
            zz[:, pl.ds(i * fb, fb)], y[...], dims, preferred_element_type=F32)
        out(1, i).start()
    for i in range(n):
        out(0, i).wait()
        out(1, i).wait()


def solution(mesh):
    def body(x, dy, w1, w2):
        rows, h = x.shape
        f = w1.shape[1]
        n = 8 * rows
        vm = pltpu.VMEM
        sem = pltpu.SemaphoreType.DMA
        vspec = pl.BlockSpec(memory_space=vm)
        hbm = pl.BlockSpec(memory_space=pltpu.HBM)
        xg, yg, zg, dzg, acc, last, mid = pl.pallas_call(
            lambda *refs: _gather_kernel(rows, *refs),
            out_shape=(vm((n, h), BF16), vm((n, h), BF16), vm((n, f), BF16), vm((n, f), BF16),
                       vm((rows, h), F32), vm((rows, h), BF16), vm((rows, h), BF16)),
            in_specs=[hbm] * 4,
            out_specs=(vspec,) * 7,
            scratch_shapes=[
                vm((n, f), F32),
                vm((h, f), BF16), vm((f, h), BF16), vm((f, h), BF16), vm((h, f), BF16),
                vm((n, h), F32), vm((4, rows, h), BF16), vm((4, rows, h), BF16),
                vm((3, rows, h), BF16), vm((2, rows, h), BF16),
                sem((2,)), sem(((f + h) // 256,)), sem(()), sem((3, 4)), sem((3, 4)), sem((5,)), sem((3,)),
            ],
            compiler_params=pltpu.CompilerParams(
                collective_id=0, has_side_effects=True, vmem_limit_bytes=40 * MIB),
            name='gather_dx',
        )(*(pltpu.with_memory_space_constraint(a, pltpu.HBM) for a in (x, dy, w1, w2)))
        mid = lax.ppermute(mid, 'tp', [(0, 1), (1, 0), (2, 4), (3, 5), (4, 2), (5, 3), (6, 7), (7, 6)])
        hops = ((0, 2), (2, 3), (3, 1), (1, 0))
        far = lax.ppermute(last, 'tp', [(2 * a + c, 2 * b + c) for a, b in hops for c in (0, 1)])
        steps = 8
        dw1, dw2 = pl.pallas_call(
            _dw_kernel,
            out_shape=(jax.ShapeDtypeStruct((h, f), F32), jax.ShapeDtypeStruct((f, h), F32)),
            in_specs=[vspec] * 4,
            out_specs=(hbm,) * 2,
            scratch_shapes=[vm((h, f), F32), vm((f, h), F32), sem((2, steps))],
            compiler_params=pltpu.CompilerParams(vmem_limit_bytes=24 * MIB),
            cost_estimate=pl.CostEstimate(
                flops=4 * n * h * f, bytes_accessed=8 * h * f, transcendentals=0),
            name='dw',
        )(xg, dzg, zg, yg)
        dx = (acc + far.astype(F32) + mid.astype(F32)).astype(BF16)
        return dx, dw1, dw2

    return jax.shard_map(
        body, mesh=mesh,
        in_specs=(P(('dp', 'tp'), None), P(('dp', 'tp'), None), P(None, 'tp'), P('tp', None)),
        out_specs=(P(('dp', 'tp'), None), P('dp', 'tp'), P(('dp', 'tp'), None)),
        check_vma=False)
```

```python
import math

import jax
import jax.numpy as jnp
from jax import lax
from jax.experimental import pallas as pl
from jax.experimental.pallas import tpu as pltpu
from jax.sharding import PartitionSpec as P


C0 = math.sqrt(2.0 / math.pi)
C1 = 0.044715
BF16 = jnp.bfloat16
F32 = jnp.float32
X, Y, Y0, Y1 = range(4)
MESH = pl.DeviceIdType.MESH
TN = (((0,), (0,)), ((), ()))
MIB = 1 << 20


def _gelu(u):
    t = jnp.tanh(C0 * (u + C1 * u * u * u))
    return 0.5 * u * (1.0 + t), 0.5 * (1.0 + t) + 0.5 * u * (1.0 - t * t) * C0 * (1.0 + 3.0 * C1 * u * u)


def _gather_kernel(rows, x_hbm, y_hbm, w1_hbm, w2_hbm,
                   xg, yg, zs, dzs, acc_ref, last_ref, mid_ref, pre_ref,
                   g1s, w1, w2, w1t, w2t, pdx, psend, precv, rsend, rrecv,
                   in_sem, w_sem, ag_send, ag_recv, ag_precv, p_recv, r_recv, met):
    t = lax.axis_index('tp')
    z, c = t // 2, t % 2
    chunk = 2 * rows
    f, h = w2.shape
    low = z < 2
    near_end, near_mid = jnp.where(low, 0, 3), jnp.where(low, 1, 2)
    far_mid, far_end = 3 - near_mid, 3 - near_end
    is_end = z == near_end
    is_mid = jnp.logical_not(is_end)

    def dev(chip, core):
        return {'tp': 2 * chip + core}

    def block(a, slot, core):
        r = pl.ds(pl.multiple_of(slot * chunk + core * rows, rows), rows)
        if a in (X, Y):
            return (xg, yg)[a].at[r, :]
        return yg.at[r, pl.ds((a - Y0) * (h // 2), h // 2)]

    def flag(a, slot):
        return {X: slot, Y: 4 + slot, Y0: 4 + slot, Y1: 8}[a]

    loads = [pltpu.make_async_copy(src, block(a, 0, c), in_sem.at[a]) for a, src in ((X, x_hbm), (Y, y_hbm))]
    wloads = []
    for hbm, w, n in ((w2_hbm, w2, 4), (w1_hbm, w1, 2)):
        for i in range(n):
            r = pl.ds(i * (w.shape[0] // n), w.shape[0] // n)
            wloads.append(pltpu.make_async_copy(hbm.at[r, :], w.at[r, :], w_sem.at[len(wloads)]))
    for cp in loads:
        cp.start()

    barrier = pltpu.get_barrier_semaphore()

    def greet(chip, core):
        pl.semaphore_signal(barrier, inc=1, device_id=dev(chip, core), device_id_type=MESH)

    greet(z, 1 - c)

    @pl.when(is_end)
    def _():
        greet(near_mid, c)

    @pl.when(is_mid)
    def _():
        greet(near_end, c)
        greet(far_end, c)

    low_mid = z == 1

    @pl.when(low_mid)
    def _():
        greet(far_mid, c)

    for cp in loads:
        cp.wait()
    for cp in wloads:
        cp.start()

    @pl.when(low_mid)
    def _():
        pl.semaphore_wait(barrier, 2)

    @pl.when(jnp.logical_not(low_mid))
    def _():
        pl.semaphore_wait(barrier, 3)

    def ag_copy(a, slot, chip, to_slot):
        return pltpu.make_async_remote_copy(
            src_ref=block(a, slot, c), dst_ref=block(a, to_slot, c),
            send_sem=ag_send, recv_sem=ag_recv.at[flag(a, to_slot) - 1],
            device_id=dev(chip, c), device_id_type=MESH)

    def share(a, slot):
        return pltpu.make_async_remote_copy(
            src_ref=block(a, slot, c), dst_ref=block(a, slot, c),
            send_sem=ag_send, recv_sem=ag_precv.at[flag(a, slot)],
            device_id=dev(z, 1 - c), device_id_type=MESH)

    def end_msg(a, i):
        return ag_copy(a, 0, *((far_mid, 1), (near_mid, 3))[i])

    def mid_msg(a, i):
        return ag_copy(a, *((0, near_end, 1), (0, far_mid, 2), (1, near_end, 2), (2, near_end, 3))[i])

    def arrive(a, slot, forward=None):
        dst = block(a, slot, c)
        pltpu.make_async_copy(dst, dst, ag_recv.at[flag(a, slot) - 1]).wait()
        if forward is not None:
            mid_msg(a, forward).start()
        share(a, slot).start()

    def partner(a, slot):
        share(a, slot).wait_recv()

    def step_u(slot, m=1, half=None):
        r = pl.ds(slot * chunk, m * chunk)
        nb = f if half is None else f // 2

        @pl.loop(half or 0, (half or 0) + 1)
        def _(n):
            s = pl.ds(pl.multiple_of(n * nb, nb), nb)
            u = jnp.dot(xg[r, :], w1[:, s], preferred_element_type=F32).astype(BF16)
            g0, g1 = _gelu(u.astype(F32))
            zs[r, s] = g0.astype(BF16)
            g1s[r, s] = g1

    def step_g(slot, m=1):
        r = pl.ds(slot * chunk, m * chunk)

        @pl.loop(0, f // 1024)
        def _(n):
            s = pl.ds(pl.multiple_of(n * 1024, 1024), 1024)
            g = jnp.dot(yg[r, :], w2t[:, s], preferred_element_type=F32)
            dzs[r, s] = (g * g1s[r, s]).astype(BF16)

    def half_g(slot, i):
        r = pl.ds(slot * chunk, chunk)
        kk = pl.ds(i * (h // 2), h // 2)

        @pl.loop(0, f // 1024)
        def _(n):
            s = pl.ds(pl.multiple_of(n * 1024, 1024), 1024)
            g = jnp.dot(yg[r, kk], w2t[kk, s], preferred_element_type=F32)
            if i == 0:
                pdx[r, s] = g
            else:
                dzs[r, s] = ((g + pdx[r, s]) * g1s[r, s]).astype(BF16)

    def step_dx(slot, m=1, half=None):
        r = pl.ds(slot * chunk, m * chunk)
        per = h // 1024 if half is None else h // 2048

        @pl.loop(0, per)
        def _(n):
            s = pl.ds(pl.multiple_of(((half or 0) * per + n) * 1024, 1024), 1024)
            pdx[r, s] = jnp.dot(dzs[r, :], w1t[:, s], preferred_element_type=F32)
            for k in range(slot, slot + m):
                psend[k, :, s] = part(k, 1 - c, s).astype(BF16)
                pair_copy(k, s, half).start()

    def first_dw():
        @pl.loop(0, pre_ref.shape[0] // 256)
        def _(n):
            s = pl.ds(pl.multiple_of(n * 256, 256), 256)
            pre_ref[s, :] = lax.dot_general(xg[:, s], dzs[...], TN, preferred_element_type=F32)

    def part(k, core, s=slice(None)):
        return pdx[pl.ds(pl.multiple_of(k * chunk + core * rows, rows), rows), s]

    def cols(half):
        return slice(None) if half is None else pl.ds(half * (h // 2), h // 2)

    def pair_copy(k, s, half=None):
        return pltpu.make_async_remote_copy(
            src_ref=psend.at[k, :, s], dst_ref=precv.at[k, :, s], send_sem=ag_send,
            recv_sem=p_recv.at[4 if half == 1 else k],
            device_id=dev(z, 1 - c), device_id_type=MESH)

    def pair_sum(k, half=None):
        s = cols(half)
        pair_copy(k, s, half).wait_recv()
        return part(k, c, s) + precv[k, :, s].astype(F32)

    def rs_copy(k, chip, i, half=None):
        s = cols(half)
        return pltpu.make_async_remote_copy(
            src_ref=rsend.at[k, :, s], dst_ref=rrecv.at[i, :, s], send_sem=ag_send,
            recv_sem=r_recv.at[2 if half == 1 else i],
            device_id=dev(chip, c), device_id_type=MESH)

    def rs_recv(i, half=None):
        s = cols(half)
        dst = rrecv.at[i, :, s]
        pltpu.make_async_copy(dst, dst, r_recv.at[2 if half == 1 else i]).wait()
        return rrecv[i, :, s].astype(F32)

    def drain(n):
        for r in (xg, yg, xg.at[pl.ds(0, (n + 12 - 16) * rows), :]):
            pltpu.make_async_copy(r, r, ag_send).wait()

    @pl.when(is_end)
    def _():
        end_msg(X, 0).start()

    @pl.when(is_mid)
    def _():
        mid_msg(X, 0).start()

        @pl.when(jnp.logical_not(low_mid))
        def _():
            pl.semaphore_signal(met, inc=1, device_id=dev(far_mid, c), device_id_type=MESH)

    share(X, 0).start()
    share(Y, 0).start()

    for i in range(4):
        wloads[i].wait()
        r = pl.ds(i * (f // 4), f // 4)
        w2t[:, r] = w2[r, :].T

    @pl.when(is_end)
    def _():
        end_msg(Y, 0).start()

    @pl.when(is_mid)
    def _():
        mid_msg(Y, 0).start()

    for i in range(8):
        if i % 4 == 0:
            wloads[4 + i // 4].wait()
        r = pl.ds(i * (h // 8), h // 8)
        w1t[:, r] = w1[r, :].T

    @pl.when(is_end)
    def _():
        partner(X, 0)
        arrive(X, 1)
        partner(X, 1)
        step_u(0, 2)
        end_msg(X, 1).start()
        arrive(Y, 1)
        partner(Y, 0)
        partner(Y, 1)
        step_g(0, 2)
        end_msg(Y, 1).start()
        step_dx(0, 2)
        arrive(X, 2)
        partner(X, 2)
        step_u(2)
        arrive(Y, 2)
        acc_ref[...] = pair_sum(0)
        rsend[1] = pair_sum(1).astype(BF16)
        rs_copy(1, near_mid, 0).start()
        partner(Y, 2)
        step_g(2)
        for i in (0, 1):
            step_dx(2, half=i)
        arrive(X, 3)
        for i in (0, 1):
            rsend[2, :, cols(i)] = pair_sum(2, i).astype(BF16)
            rs_copy(2, far_end, 0, i).start()

        @pl.when(c == 1)
        def _():
            arrive(Y0, 3)
            partner(X, 3)
            step_u(3, half=0)
            arrive(Y1, 3)
            step_u(3, half=1)
            partner(Y0, 3)
            half_g(3, 0)

        @pl.when(c == 0)
        def _():
            partner(X, 3)
            step_u(3)
            arrive(Y0, 3)
            partner(Y0, 3)
            half_g(3, 0)
            arrive(Y1, 3)

        partner(Y1, 3)
        half_g(3, 1)
        step_dx(3)
        first_dw()
        mid_ref[...] = jnp.zeros_like(mid_ref)
        last_ref[...] = pair_sum(3).astype(BF16)
        for i in (0, 1):
            acc_ref[:, cols(i)] += rs_recv(0, i)
        drain(4 + 2)

    @pl.when(is_mid)
    def _():
        partner(X, 0)
        step_u(0)
        arrive(X, 1, forward=2)

        @pl.when(low_mid)
        def _():
            pl.semaphore_wait(met, 1)

        mid_msg(X, 1).start()

        @pl.when(low)
        def _():
            arrive(Y, 1, forward=2)
            mid_msg(Y0, 1).start()

        partner(X, 1)
        step_u(1)

        @pl.when(jnp.logical_not(low))
        def _():
            mid_msg(Y0, 1).start()
            arrive(Y, 1, forward=2)

        mid_msg(Y1, 1).start()
        partner(Y, 0)
        partner(Y, 1)
        step_g(0, 2)
        arrive(X, 2, forward=3)
        arrive(X, 3)
        step_dx(0, 2)
        arrive(Y0, 2, forward=3)
        acc_ref[...] = pair_sum(0)
        rsend[1] = pair_sum(1).astype(BF16)

        @pl.when(low)
        def _():
            rs_copy(1, far_mid, 1).start()

        arrive(Y1, 2, forward=3)

        @pl.when(jnp.logical_not(low))
        def _():
            rs_copy(1, far_mid, 1).start()

        partner(X, 2)
        partner(X, 3)
        step_u(2, 2)
        arrive(Y, 3)
        partner(Y0, 2)
        partner(Y1, 2)
        partner(Y, 3)
        step_g(2, 2)
        step_dx(2, 2)
        first_dw()
        mid_ref[...] = pair_sum(2).astype(BF16)
        last_ref[...] = (pair_sum(3) + rs_recv(1)).astype(BF16)
        acc_ref[...] += rs_recv(0)
        drain(8 + 1)


def _dw_kernel(x, dz, zz, y, pre, dw1, dw2, b1, b2, sem):
    n = sem.shape[1]
    hb, fb = x.shape[1] // n, zz.shape[1] // n

    def out(j, i):
        src, dst, m = ((b1, dw1, hb), (b2, dw2, fb))[j]
        s = pl.ds(i * m, m)
        if j == 0 and (i + 1) * hb <= pre.shape[0]:
            src = pre
        return pltpu.make_async_copy(src.at[s, :], dst.at[s, :], sem.at[j, i])

    done = pre.shape[0] // hb
    for i in range(done):
        out(0, i).start()
    for i in range(n):
        b2[pl.ds(i * fb, fb), :] = lax.dot_general(
            zz[:, pl.ds(i * fb, fb)], y[...], TN, preferred_element_type=F32)
        out(1, i).start()
        if i >= done:
            b1[pl.ds(i * hb, hb), :] = lax.dot_general(
                x[:, pl.ds(i * hb, hb)], dz[...], TN, preferred_element_type=F32)
            out(0, i).start()
    for i in range(n):
        out(0, i).wait()
        out(1, i).wait()


def solution(mesh):
    def body(x, dy, w1, w2):
        rows, h = x.shape
        f = w1.shape[1]
        n = 8 * rows
        vm = pltpu.VMEM
        sem = pltpu.SemaphoreType.DMA
        vspec = pl.BlockSpec(memory_space=vm)
        hbm = pl.BlockSpec(memory_space=pltpu.HBM)
        xg, yg, zg, dzg, acc, last, mid, pre = pl.pallas_call(
            lambda *refs: _gather_kernel(rows, *refs),
            out_shape=(vm((n, h), BF16), vm((n, h), BF16), vm((n, f), BF16), vm((n, f), BF16),
                       vm((rows, h), F32), vm((rows, h), BF16), vm((rows, h), BF16), vm((h // 4, f), F32)),
            in_specs=[hbm] * 4,
            out_specs=(vspec,) * 8,
            scratch_shapes=[
                vm((n, f), F32),
                vm((h, f), BF16), vm((f, h), BF16), vm((f, h), BF16), vm((h, f), BF16),
                vm((n, h), F32), vm((4, rows, h), BF16), vm((4, rows, h), BF16),
                vm((3, rows, h), BF16), vm((2, rows, h), BF16),
                sem((2,)), sem((6,)), sem(()), sem((8,)), sem((9,)), sem((5,)), sem((3,)), pltpu.SemaphoreType.REGULAR,
            ],
            compiler_params=pltpu.CompilerParams(
                collective_id=0, has_side_effects=True, vmem_limit_bytes=40 * MIB),
            name='gather_dx',
        )(*(pltpu.with_memory_space_constraint(a, pltpu.HBM) for a in (x, dy, w1, w2)))
        mid = lax.ppermute(mid, 'tp', [(0, 1), (1, 0), (2, 4), (3, 5), (4, 2), (5, 3), (6, 7), (7, 6)])
        hops = ((0, 2), (2, 3), (3, 1), (1, 0))
        far = lax.ppermute(last, 'tp', [(2 * a + c, 2 * b + c) for a, b in hops for c in (0, 1)])
        steps = 8
        dw1, dw2 = pl.pallas_call(
            _dw_kernel,
            out_shape=(jax.ShapeDtypeStruct((h, f), F32), jax.ShapeDtypeStruct((f, h), F32)),
            in_specs=[vspec] * 5,
            out_specs=(hbm,) * 2,
            scratch_shapes=[vm((h, f), F32), vm((f, h), F32), sem((2, steps))],
            compiler_params=pltpu.CompilerParams(vmem_limit_bytes=24 * MIB),
            cost_estimate=pl.CostEstimate(
                flops=4 * n * h * f, bytes_accessed=8 * h * f, transcendentals=0),
            name='dw',
        )(xg, dzg, zg, yg, pre)
        dx = (acc + far.astype(F32) + mid.astype(F32)).astype(BF16)
        return dx, dw1, dw2

    return jax.shard_map(
        body, mesh=mesh,
        in_specs=(P(('dp', 'tp'), None), P(('dp', 'tp'), None), P(None, 'tp'), P('tp', None)),
        out_specs=(P(('dp', 'tp'), None), P('dp', 'tp'), P(('dp', 'tp'), None)),
        check_vma=False)
```

```python
import math

import jax
import jax.numpy as jnp
from jax import lax
from jax.experimental import pallas as pl
from jax.experimental.pallas import tpu as pltpu
from jax.sharding import PartitionSpec as P


C0 = math.sqrt(2.0 / math.pi)
C1 = 0.044715
BF16 = jnp.bfloat16
F32 = jnp.float32
X, Y, Y0, Y1 = range(4)
MESH = pl.DeviceIdType.MESH
TN = (((0,), (0,)), ((), ()))
MIB = 1 << 20


def _gelu(u):
    t = jnp.tanh(C0 * (u + C1 * u * u * u))
    return 0.5 * u * (1.0 + t), 0.5 * (1.0 + t) + 0.5 * u * (1.0 - t * t) * C0 * (1.0 + 3.0 * C1 * u * u)


def _gather_kernel(rows, x_hbm, y_hbm, w1_hbm, w2_hbm,
                   xg, yg, zs, dzs, acc_ref, last_ref, mid_ref, pre_ref,
                   g1s, w1, w2, w1t, w2t, pdx, psend, precv, rsend, rrecv,
                   in_sem, w_sem, ag_send, ag_recv, ag_precv, p_recv, r_recv, met):
    t = lax.axis_index('tp')
    z, c = t // 2, t % 2
    chunk = 2 * rows
    f, h = w2.shape
    low = z < 2
    near_end, near_mid = jnp.where(low, 0, 3), jnp.where(low, 1, 2)
    far_mid, far_end = 3 - near_mid, 3 - near_end
    is_end = z == near_end
    is_mid = jnp.logical_not(is_end)
    parts = ((0, 512), (512, 512), (1024, 1024))

    def dev(chip, core):
        return {'tp': 2 * chip + core}

    def block(a, slot, core):
        r = pl.ds(pl.multiple_of(slot * chunk + core * rows, rows), rows)
        if a in (X, Y):
            return (xg, yg)[a].at[r, :]
        return yg.at[r, pl.ds((a - Y0) * (h // 2), h // 2)]

    def flag(a, slot):
        return {X: 2 * slot, Y: 2 * slot + 1, Y0: 2 * slot + 1, Y1: 8}[a]

    loads = [pltpu.make_async_copy(src, block(a, 0, c), in_sem) for a, src in ((X, x_hbm), (Y, y_hbm))]
    wloads = []
    for hbm, w, n in ((w2_hbm, w2, 4), (w1_hbm, w1, 2)):
        for i in range(n):
            r = pl.ds(i * (w.shape[0] // n), w.shape[0] // n)
            wloads.append(pltpu.make_async_copy(hbm.at[r, :], w.at[r, :], w_sem.at[len(wloads)]))
    for cp in loads:
        cp.start()

    barrier = pltpu.get_barrier_semaphore()

    def greet(chip, core):
        pl.semaphore_signal(barrier, inc=1, device_id=dev(chip, core), device_id_type=MESH)

    greet(z, 1 - c)

    @pl.when(is_end)
    def _():
        greet(near_mid, c)

    @pl.when(is_mid)
    def _():
        greet(near_end, c)
        greet(far_end, c)

    low_mid = z == 1

    @pl.when(low_mid)
    def _():
        greet(far_mid, c)

    both = xg.at[pl.ds(0, chunk), :]
    pltpu.make_async_copy(both, both, in_sem).wait()
    for cp in wloads:
        cp.start()

    @pl.when(low_mid)
    def _():
        pl.semaphore_wait(barrier, 2)

    @pl.when(jnp.logical_not(low_mid))
    def _():
        pl.semaphore_wait(barrier, 3)

    def ag_copy(a, slot, chip, to_slot):
        return pltpu.make_async_remote_copy(
            src_ref=block(a, slot, c), dst_ref=block(a, to_slot, c),
            send_sem=ag_send, recv_sem=ag_recv.at[flag(a, to_slot) - 2],
            device_id=dev(chip, c), device_id_type=MESH)

    def share(a, slot):
        return pltpu.make_async_remote_copy(
            src_ref=block(a, slot, c), dst_ref=block(a, slot, c),
            send_sem=ag_send, recv_sem=ag_precv.at[flag(a, slot)],
            device_id=dev(z, 1 - c), device_id_type=MESH)

    def end_msg(a, i):
        return ag_copy(a, 0, *((far_mid, 1), (near_mid, 3))[i])

    def mid_msg(a, i):
        return ag_copy(a, *((0, near_end, 1), (0, far_mid, 2), (1, near_end, 2), (2, near_end, 3))[i])

    def arrive(a, slot, forward=None):
        dst = block(a, slot, c)
        pltpu.make_async_copy(dst, dst, ag_recv.at[flag(a, slot) - 2]).wait()
        if forward is not None:
            mid_msg(a, forward).start()
        share(a, slot).start()

    def partner(a, slot):
        share(a, slot).wait_recv()

    def step_u(slot, m=1, half=None):
        r = pl.ds(slot * chunk, m * chunk)
        nb = f // 2

        @pl.loop(half or 0, 2 if half is None else half + 1)
        def _(n):
            s = pl.ds(pl.multiple_of(n * nb, nb), nb)
            u = jnp.dot(xg[r, :], w1[:, s], preferred_element_type=F32).astype(BF16)
            g0, g1 = _gelu(u.astype(F32))
            zs[r, s] = g0.astype(BF16)
            g1s[r, s] = g1

    def step_g(slot, m=1):
        r = pl.ds(slot * chunk, m * chunk)

        @pl.loop(0, f // 1024)
        def _(n):
            s = pl.ds(pl.multiple_of(n * 1024, 1024), 1024)
            g = jnp.dot(yg[r, :], w2t[:, s], preferred_element_type=F32)
            dzs[r, s] = (g * g1s[r, s]).astype(BF16)

    def half_g(slot, i):
        r = pl.ds(slot * chunk, chunk)
        kk = pl.ds(i * (h // 2), h // 2)

        @pl.loop(0, f // 1024)
        def _(n):
            s = pl.ds(pl.multiple_of(n * 1024, 1024), 1024)
            g = jnp.dot(yg[r, kk], w2t[kk, s], preferred_element_type=F32)
            if i == 0:
                pdx[r, s] = g
            else:
                dzs[r, s] = ((g + pdx[r, s]) * g1s[r, s]).astype(BF16)

    def step_dx(slot, m=1, half=None):
        r = pl.ds(slot * chunk, m * chunk)
        first, n, nb = (0, h // 1024, 1024) if half is None else (parts[half][0], 1, parts[half][1])

        @pl.loop(0, n)
        def _(n):
            s = pl.ds(pl.multiple_of(first + n * nb, nb if half is None else 128), nb)
            pdx[r, s] = jnp.dot(dzs[r, :], w1t[:, s], preferred_element_type=F32)
            for k in range(slot, slot + m):
                psend[k, :, s] = part(k, 1 - c, s).astype(BF16)
                pair_copy(k, s, half).start()

    def first_dw():
        @pl.loop(0, pre_ref.shape[0] // 256)
        def _(n):
            s = pl.ds(pl.multiple_of(n * 256, 256), 256)
            pre_ref[s, :] = lax.dot_general(xg[:, s], dzs[...], TN, preferred_element_type=F32)

    def part(k, core, s=slice(None)):
        return pdx[pl.ds(pl.multiple_of(k * chunk + core * rows, rows), rows), s]

    def cols(half):
        return slice(None) if half is None else pl.ds(*parts[half])

    def pair_copy(k, s, half=None):
        return pltpu.make_async_remote_copy(
            src_ref=psend.at[k, :, s], dst_ref=precv.at[k, :, s], send_sem=ag_send,
            recv_sem=p_recv.at[3 + half if half else k],
            device_id=dev(z, 1 - c), device_id_type=MESH)

    def pair_sum(k, half=None):
        s = cols(half)
        pair_copy(k, s, half).wait_recv()
        return part(k, c, s) + precv[k, :, s].astype(F32)

    def rs_copy(k, chip, i, half=None):
        s = cols(half)
        return pltpu.make_async_remote_copy(
            src_ref=rsend.at[k, :, s], dst_ref=rrecv.at[i, :, s], send_sem=ag_send,
            recv_sem=r_recv.at[1 + half if half else i],
            device_id=dev(chip, c), device_id_type=MESH)

    def rs_recv(i, half=None):
        s = cols(half)
        dst = rrecv.at[i, :, s]
        pltpu.make_async_copy(dst, dst, r_recv.at[1 + half if half else i]).wait()
        return rrecv[i, :, s].astype(F32)

    def drain(n):
        for r in (xg, yg, xg.at[pl.ds(0, (n + 12 - 16) * rows), :]):
            pltpu.make_async_copy(r, r, ag_send).wait()

    @pl.when(is_end)
    def _():
        end_msg(X, 0).start()

    @pl.when(is_mid)
    def _():
        mid_msg(X, 0).start()

        @pl.when(jnp.logical_not(low_mid))
        def _():
            pl.semaphore_signal(met, inc=1, device_id=dev(far_mid, c), device_id_type=MESH)

    share(X, 0).start()
    share(Y, 0).start()

    for i in range(4):
        wloads[i].wait()
        r = pl.ds(i * (f // 4), f // 4)
        w2t[:, r] = w2[r, :].T

    @pl.when(is_end)
    def _():
        end_msg(Y, 0).start()

    @pl.when(is_mid)
    def _():
        mid_msg(Y, 0).start()

    for i in range(8):
        if i % 4 == 0:
            wloads[4 + i // 4].wait()
        r = pl.ds(i * (h // 8), h // 8)
        w1t[:, r] = w1[r, :].T

    @pl.when(is_mid)
    def _():
        partner(X, 0)
        step_u(0)
        arrive(X, 1, forward=2)

        @pl.when(low_mid)
        def _():
            pl.semaphore_wait(met, 1)

        mid_msg(X, 1).start()

        @pl.when(low)
        def _():
            arrive(Y, 1, forward=2)
            mid_msg(Y0, 1).start()

        partner(X, 1)
        step_u(1)

        @pl.when(jnp.logical_not(low))
        def _():
            mid_msg(Y0, 1).start()
            arrive(Y, 1, forward=2)

        mid_msg(Y1, 1).start()
        partner(Y, 0)
        partner(Y, 1)
        step_g(0, 2)
        arrive(X, 2, forward=3)
        arrive(X, 3)
        step_dx(0, 2)
        arrive(Y0, 2, forward=3)
        acc_ref[...] = pair_sum(0)
        rsend[1] = pair_sum(1).astype(BF16)

        rs_copy(1, far_mid, 1).start()
        arrive(Y1, 2, forward=3)
        partner(X, 2)
        partner(X, 3)
        step_u(2, 2)
        arrive(Y, 3)
        partner(Y0, 2)
        partner(Y1, 2)
        partner(Y, 3)
        step_g(2, 2)
        step_dx(2, 2)
        first_dw()
        mid_ref[...] = pair_sum(2).astype(BF16)
        last_ref[...] = (pair_sum(3) + rs_recv(1)).astype(BF16)
        acc_ref[...] += rs_recv(0)
        drain(8 + 1)

    @pl.when(is_end)
    def _():
        partner(X, 0)
        arrive(X, 1)
        partner(X, 1)
        step_u(0, 2)
        end_msg(X, 1).start()
        arrive(Y, 1)
        partner(Y, 0)
        partner(Y, 1)
        step_g(0, 2)
        end_msg(Y, 1).start()
        step_dx(0, 2)
        arrive(X, 2)
        partner(X, 2)
        step_u(2)
        arrive(Y, 2)
        acc_ref[...] = pair_sum(0)
        rsend[1] = pair_sum(1).astype(BF16)
        rs_copy(1, near_mid, 0).start()
        partner(Y, 2)
        step_g(2)
        for i in range(len(parts)):
            step_dx(2, half=i)
        rsend[2, :, cols(0)] = pair_sum(2, 0).astype(BF16)
        rs_copy(2, far_end, 0, 0).start()
        arrive(X, 3)
        for i in range(1, len(parts)):
            rsend[2, :, cols(i)] = pair_sum(2, i).astype(BF16)
            rs_copy(2, far_end, 0, i).start()

        @pl.when(c == 1)
        def _():
            arrive(Y0, 3)
            arrive(Y1, 3)
            partner(X, 3)
            step_u(3)
            partner(Y0, 3)
            half_g(3, 0)

        @pl.when(c == 0)
        def _():
            partner(X, 3)
            step_u(3)
            arrive(Y0, 3)
            partner(Y0, 3)
            half_g(3, 0)
            arrive(Y1, 3)

        partner(Y1, 3)
        half_g(3, 1)
        step_dx(3)
        first_dw()
        mid_ref[...] = jnp.zeros_like(mid_ref)
        last_ref[...] = pair_sum(3).astype(BF16)
        for i in range(len(parts)):
            acc_ref[:, cols(i)] += rs_recv(0, i)
        drain(4 + 2)


def _dw_kernel(x, dz, zz, y, pre, dw1, dw2, b1, b2, sem):
    n = sem.shape[1]
    hb, fb = x.shape[1] // n, zz.shape[1] // n

    def out(j, i):
        src, dst, m = ((b1, dw1, hb), (b2, dw2, fb))[j]
        s = pl.ds(i * m, m)
        if j == 0 and (i + 1) * hb <= pre.shape[0]:
            src = pre
        return pltpu.make_async_copy(src.at[s, :], dst.at[s, :], sem.at[j, i])

    done = pre.shape[0] // hb
    for i in range(done):
        out(0, i).start()
    for i in range(n):
        b2[pl.ds(i * fb, fb), :] = lax.dot_general(
            zz[:, pl.ds(i * fb, fb)], y[...], TN, preferred_element_type=F32)
        out(1, i).start()
        if i >= done:
            b1[pl.ds(i * hb, hb), :] = lax.dot_general(
                x[:, pl.ds(i * hb, hb)], dz[...], TN, preferred_element_type=F32)
            out(0, i).start()
    for i in range(n):
        out(0, i).wait()
        out(1, i).wait()


def solution(mesh):
    def body(x, dy, w1, w2):
        rows, h = x.shape
        f = w1.shape[1]
        n = 8 * rows
        vm = pltpu.VMEM
        sem = pltpu.SemaphoreType.DMA
        vspec = pl.BlockSpec(memory_space=vm)
        hbm = pl.BlockSpec(memory_space=pltpu.HBM)
        xg, yg, zg, dzg, acc, last, mid, pre = pl.pallas_call(
            lambda *refs: _gather_kernel(rows, *refs),
            out_shape=(vm((n, h), BF16), vm((n, h), BF16), vm((n, f), BF16), vm((n, f), BF16),
                       vm((rows, h), F32), vm((rows, h), BF16), vm((rows, h), BF16), vm((h // 4, f), F32)),
            in_specs=[hbm] * 4,
            out_specs=(vspec,) * 8,
            scratch_shapes=[
                vm((n, f), F32),
                vm((h, f), BF16), vm((f, h), BF16), vm((f, h), BF16), vm((h, f), BF16),
                vm((n, h), F32), vm((4, rows, h), BF16), vm((4, rows, h), BF16),
                vm((3, rows, h), BF16), vm((2, rows, h), BF16),
                sem(()), sem((6,)), sem(()), sem((7,)), sem((9,)), sem((6,)), sem((4,)), pltpu.SemaphoreType.REGULAR,
            ],
            compiler_params=pltpu.CompilerParams(
                collective_id=0, has_side_effects=True, vmem_limit_bytes=40 * MIB),
            name='gather_dx',
        )(*(pltpu.with_memory_space_constraint(a, pltpu.HBM) for a in (x, dy, w1, w2)))
        mid = lax.ppermute(mid, 'tp', [(0, 1), (1, 0), (2, 4), (3, 5), (4, 2), (5, 3), (6, 7), (7, 6)])
        hops = ((0, 2), (2, 3), (3, 1), (1, 0))
        far = lax.ppermute(last, 'tp', [(2 * a + c, 2 * b + c) for a, b in hops for c in (0, 1)])
        steps = 8
        dw1, dw2 = pl.pallas_call(
            _dw_kernel,
            out_shape=(jax.ShapeDtypeStruct((h, f), F32), jax.ShapeDtypeStruct((f, h), F32)),
            in_specs=[vspec] * 5,
            out_specs=(hbm,) * 2,
            scratch_shapes=[vm((h, f), F32), vm((f, h), F32), sem((2, steps))],
            compiler_params=pltpu.CompilerParams(vmem_limit_bytes=24 * MIB),
            cost_estimate=pl.CostEstimate(
                flops=4 * n * h * f, bytes_accessed=8 * h * f, transcendentals=0),
            name='dw',
        )(xg, dzg, zg, yg, pre)
        dx = (acc + far.astype(F32) + mid.astype(F32)).astype(BF16)
        return dx, dw1, dw2

    return jax.shard_map(
        body, mesh=mesh,
        in_specs=(P(('dp', 'tp'), None), P(('dp', 'tp'), None), P(None, 'tp'), P('tp', None)),
        out_specs=(P(('dp', 'tp'), None), P('dp', 'tp'), P(('dp', 'tp'), None)),
        check_vma=False)
```

```python
import math

import jax
import jax.numpy as jnp
from jax import lax
from jax.experimental import pallas as pl
from jax.experimental.pallas import tpu as pltpu
from jax.sharding import PartitionSpec as P


C0 = math.sqrt(2.0 / math.pi)
C1 = 0.044715
BF16 = jnp.bfloat16
F32 = jnp.float32
X, Y, Y0, Y1 = range(4)
MESH = pl.DeviceIdType.MESH
TN = (((0,), (0,)), ((), ()))
MIB = 1 << 20


def _gelu(u):
    t = jnp.tanh(C0 * (u + C1 * u * u * u))
    return 0.5 * u * (1.0 + t), 0.5 * (1.0 + t) + 0.5 * u * (1.0 - t * t) * C0 * (1.0 + 3.0 * C1 * u * u)


def _gather_kernel(rows, x_hbm, y_hbm, w1_hbm, w2_hbm,
                   xg, yg, zs, dzs, acc_ref, last_ref, mid_ref, pre_ref,
                   g1s, w1, w2, w1t, w2t, pdx, psend, precv, rsend, rrecv,
                   in_sem, w_sem, ag_send, ag_recv, ag_precv, p_recv, r_recv, met):
    t = lax.axis_index('tp')
    z, c = t // 2, t % 2
    chunk = 2 * rows
    f, h = w2.shape
    low = z < 2
    near_end, near_mid = jnp.where(low, 0, 3), jnp.where(low, 1, 2)
    far_mid, far_end = 3 - near_mid, 3 - near_end
    is_end = z == near_end
    is_mid = jnp.logical_not(is_end)
    parts = ((0, 512), (512, 512), (1024, 1024))

    def dev(chip, core):
        return {'tp': 2 * chip + core}

    def block(a, slot, core):
        r = pl.ds(pl.multiple_of(slot * chunk + core * rows, rows), rows)
        if a in (X, Y):
            return (xg, yg)[a].at[r, :]
        return yg.at[r, pl.ds((a - Y0) * (h // 2), h // 2)]

    def flag(a, slot):
        return {X: 2 * slot, Y: 2 * slot + 1, Y0: 2 * slot + 1, Y1: 8}[a]

    loads = [pltpu.make_async_copy(src, block(a, 0, c), in_sem) for a, src in ((X, x_hbm), (Y, y_hbm))]
    wloads = []
    for hbm, w, n in ((w2_hbm, w2, 4), (w1_hbm, w1, 2)):
        for i in range(n):
            r = pl.ds(i * (w.shape[0] // n), w.shape[0] // n)
            wloads.append(pltpu.make_async_copy(hbm.at[r, :], w.at[r, :], w_sem.at[len(wloads)]))
    for cp in loads:
        cp.start()

    barrier = pltpu.get_barrier_semaphore()

    def greet(chip, core):
        pl.semaphore_signal(barrier, inc=1, device_id=dev(chip, core), device_id_type=MESH)

    greet(z, 1 - c)

    @pl.when(is_end)
    def _():
        greet(near_mid, c)

    @pl.when(is_mid)
    def _():
        greet(near_end, c)
        greet(far_end, c)

    low_mid = z == 1

    @pl.when(low_mid)
    def _():
        greet(far_mid, c)

    both = xg.at[pl.ds(0, chunk), :]
    pltpu.make_async_copy(both, both, in_sem).wait()
    for cp in wloads:
        cp.start()

    @pl.when(low_mid)
    def _():
        pl.semaphore_wait(barrier, 2)

    @pl.when(jnp.logical_not(low_mid))
    def _():
        pl.semaphore_wait(barrier, 3)

    def ag_copy(a, slot, chip, to_slot):
        return pltpu.make_async_remote_copy(
            src_ref=block(a, slot, c), dst_ref=block(a, to_slot, c),
            send_sem=ag_send, recv_sem=ag_recv.at[flag(a, to_slot) - 2],
            device_id=dev(chip, c), device_id_type=MESH)

    def share(a, slot):
        return pltpu.make_async_remote_copy(
            src_ref=block(a, slot, c), dst_ref=block(a, slot, c),
            send_sem=ag_send, recv_sem=ag_precv.at[flag(a, slot)],
            device_id=dev(z, 1 - c), device_id_type=MESH)

    def end_msg(a, i):
        return ag_copy(a, 0, *((far_mid, 1), (near_mid, 3))[i])

    def mid_msg(a, i):
        return ag_copy(a, *((0, near_end, 1), (0, far_mid, 2), (1, near_end, 2), (2, near_end, 3))[i])

    def arrive(a, slot, forward=None):
        dst = block(a, slot, c)
        pltpu.make_async_copy(dst, dst, ag_recv.at[flag(a, slot) - 2]).wait()
        if forward is not None:
            mid_msg(a, forward).start()
        share(a, slot).start()

    def partner(a, slot):
        share(a, slot).wait_recv()

    def step_u(slot, m=1, half=None):
        r = pl.ds(slot * chunk, m * chunk)
        nb = f // 2

        @pl.loop(half or 0, 2 if half is None else half + 1)
        def _(n):
            s = pl.ds(pl.multiple_of(n * nb, nb), nb)
            u = jnp.dot(xg[r, :], w1[:, s], preferred_element_type=F32).astype(BF16)
            g0, g1 = _gelu(u.astype(F32))
            zs[r, s] = g0.astype(BF16)
            g1s[r, s] = g1

    def step_g(slot, m=1):
        r = pl.ds(slot * chunk, m * chunk)

        @pl.loop(0, f // 1024)
        def _(n):
            s = pl.ds(pl.multiple_of(n * 1024, 1024), 1024)
            g = jnp.dot(yg[r, :], w2t[:, s], preferred_element_type=F32)
            dzs[r, s] = (g * g1s[r, s]).astype(BF16)

    def half_g(slot, i):
        r = pl.ds(slot * chunk, chunk)
        kk = pl.ds(i * (h // 2), h // 2)

        @pl.loop(0, f // 1024)
        def _(n):
            s = pl.ds(pl.multiple_of(n * 1024, 1024), 1024)
            g = jnp.dot(yg[r, kk], w2t[kk, s], preferred_element_type=F32)
            if i == 0:
                pdx[r, s] = g
            else:
                dzs[r, s] = ((g + pdx[r, s]) * g1s[r, s]).astype(BF16)

    def step_dx(slot, m=1, half=None):
        r = pl.ds(slot * chunk, m * chunk)
        first, n, nb = (0, h // 1024, 1024) if half is None else (parts[half][0], 1, parts[half][1])

        @pl.loop(0, n)
        def _(n):
            s = pl.ds(pl.multiple_of(first + n * nb, nb if half is None else 128), nb)
            pdx[r, s] = jnp.dot(dzs[r, :], w1t[:, s], preferred_element_type=F32)
            for k in range(slot, slot + m):
                psend[k, :, s] = part(k, 1 - c, s).astype(BF16)
                pair_copy(k, s, half).start()

    def first_dw():
        @pl.loop(0, pre_ref.shape[0] // 256)
        def _(n):
            s = pl.ds(pl.multiple_of(n * 256, 256), 256)
            pre_ref[s, :] = lax.dot_general(xg[:, s], dzs[...], TN, preferred_element_type=F32)

    def part(k, core, s=slice(None)):
        return pdx[pl.ds(pl.multiple_of(k * chunk + core * rows, rows), rows), s]

    def cols(half):
        return slice(None) if half is None else pl.ds(*parts[half])

    def pair_copy(k, s, half=None):
        return pltpu.make_async_remote_copy(
            src_ref=psend.at[k, :, s], dst_ref=precv.at[k, :, s], send_sem=ag_send,
            recv_sem=p_recv.at[3 + half if half else k],
            device_id=dev(z, 1 - c), device_id_type=MESH)

    def pair_sum(k, half=None):
        s = cols(half)
        pair_copy(k, s, half).wait_recv()
        return part(k, c, s) + precv[k, :, s].astype(F32)

    def rs_copy(k, chip, i, half=None):
        s = cols(half)
        return pltpu.make_async_remote_copy(
            src_ref=rsend.at[k, :, s], dst_ref=rrecv.at[i, :, s], send_sem=ag_send,
            recv_sem=r_recv.at[1 + half if half else i],
            device_id=dev(chip, c), device_id_type=MESH)

    def rs_recv(i, half=None):
        s = cols(half)
        dst = rrecv.at[i, :, s]
        pltpu.make_async_copy(dst, dst, r_recv.at[1 + half if half else i]).wait()
        return rrecv[i, :, s].astype(F32)

    def drain(n):
        for r in (xg, yg, xg.at[pl.ds(0, (n + 12 - 16) * rows), :]):
            pltpu.make_async_copy(r, r, ag_send).wait()

    @pl.when(is_end)
    def _():
        end_msg(X, 0).start()

    @pl.when(is_mid)
    def _():
        mid_msg(X, 0).start()

        @pl.when(jnp.logical_not(low_mid))
        def _():
            pl.semaphore_signal(met, inc=1, device_id=dev(far_mid, c), device_id_type=MESH)

    share(X, 0).start()
    share(Y, 0).start()

    for i in range(4):
        wloads[i].wait()
        r = pl.ds(i * (f // 4), f // 4)
        w2t[:, r] = w2[r, :].T

    @pl.when(is_end)
    def _():
        end_msg(Y, 0).start()

    @pl.when(is_mid)
    def _():
        mid_msg(Y, 0).start()

    for i in range(8):
        if i % 4 == 0:
            wloads[4 + i // 4].wait()
        r = pl.ds(i * (h // 8), h // 8)
        w1t[:, r] = w1[r, :].T

    @pl.when(is_mid)
    def _():
        partner(X, 0)
        step_u(0)
        arrive(X, 1, forward=2)

        @pl.when(low_mid)
        def _():
            pl.semaphore_wait(met, 1)

        mid_msg(X, 1).start()

        @pl.when(low)
        def _():
            arrive(Y, 1, forward=2)
            mid_msg(Y0, 1).start()

        partner(X, 1)
        step_u(1)

        @pl.when(jnp.logical_not(low))
        def _():
            mid_msg(Y0, 1).start()
            arrive(Y, 1, forward=2)

        mid_msg(Y1, 1).start()
        partner(Y, 0)
        partner(Y, 1)
        step_g(0, 2)
        arrive(X, 2, forward=3)
        arrive(X, 3)
        step_dx(0, 2)
        arrive(Y0, 2, forward=3)
        acc_ref[...] = pair_sum(0)
        rsend[1] = pair_sum(1).astype(BF16)

        rs_copy(1, far_mid, 1).start()
        arrive(Y1, 2, forward=3)
        partner(X, 2)
        partner(X, 3)
        step_u(2, 2)
        arrive(Y, 3)
        partner(Y0, 2)
        partner(Y1, 2)
        partner(Y, 3)
        step_g(2, 2)
        step_dx(2, 2)
        first_dw()
        mid_ref[...] = pair_sum(2).astype(BF16)
        last_ref[...] = (pair_sum(3) + rs_recv(1)).astype(BF16)
        acc_ref[...] += rs_recv(0)
        drain(8 + 1)

    @pl.when(is_end)
    def _():
        partner(X, 0)
        arrive(X, 1)
        partner(X, 1)
        step_u(0, 2)
        end_msg(X, 1).start()
        arrive(Y, 1)
        partner(Y, 0)
        partner(Y, 1)
        step_g(0, 2)
        end_msg(Y, 1).start()
        step_dx(0, 2)
        arrive(X, 2)
        partner(X, 2)
        step_u(2)
        arrive(Y, 2)
        acc_ref[...] = pair_sum(0)
        rsend[1] = pair_sum(1).astype(BF16)
        rs_copy(1, near_mid, 0).start()
        partner(Y, 2)
        step_g(2)
        for i in range(len(parts)):
            step_dx(2, half=i)
        rsend[2, :, cols(0)] = pair_sum(2, 0).astype(BF16)
        rs_copy(2, far_end, 0, 0).start()
        arrive(X, 3)
        for i in range(1, len(parts)):
            rsend[2, :, cols(i)] = pair_sum(2, i).astype(BF16)
            rs_copy(2, far_end, 0, i).start()

        @pl.when(c == 1)
        def _():
            arrive(Y0, 3)
            arrive(Y1, 3)
            partner(X, 3)
            step_u(3)
            partner(Y0, 3)
            half_g(3, 0)

        @pl.when(c == 0)
        def _():
            partner(X, 3)
            step_u(3)
            arrive(Y0, 3)
            partner(Y0, 3)
            half_g(3, 0)
            arrive(Y1, 3)

        partner(Y1, 3)
        half_g(3, 1)
        step_dx(3)
        first_dw()
        mid_ref[...] = jnp.zeros_like(mid_ref)
        last_ref[...] = pair_sum(3).astype(BF16)
        for i in range(len(parts)):
            acc_ref[:, cols(i)] += rs_recv(0, i)
        drain(4 + 2)


def _dw_kernel(x, dz, zz, y, pre, dw1, dw2, b1, b2, sem):
    n = 8
    hb, fb = x.shape[1] // n, zz.shape[1] // n

    def out(j, i):
        src, dst, m = ((b1, dw1, hb), (b2, dw2, fb))[j]
        s = pl.ds(i * m, m)
        if j == 0 and (i + 1) * hb <= pre.shape[0]:
            src = pre
        return pltpu.make_async_copy(src.at[s, :], dst.at[s, :], sem)

    done = pre.shape[0] // hb
    for i in range(done):
        out(0, i).start()
    for i in range(n):
        b2[pl.ds(i * fb, fb), :] = lax.dot_general(
            zz[:, pl.ds(i * fb, fb)], y[...], TN, preferred_element_type=F32)
        out(1, i).start()
        if i >= done:
            b1[pl.ds(i * hb, hb), :] = lax.dot_general(
                x[:, pl.ds(i * hb, hb)], dz[...], TN, preferred_element_type=F32)
            out(0, i).start()
    pltpu.make_async_copy(b1, dw1, sem).wait()
    pltpu.make_async_copy(b2, dw2, sem).wait()


def solution(mesh):
    def body(x, dy, w1, w2):
        rows, h = x.shape
        f = w1.shape[1]
        n = 8 * rows
        vm = pltpu.VMEM
        sem = pltpu.SemaphoreType.DMA
        vspec = pl.BlockSpec(memory_space=vm)
        hbm = pl.BlockSpec(memory_space=pltpu.HBM)
        xg, yg, zg, dzg, acc, last, mid, pre = pl.pallas_call(
            lambda *refs: _gather_kernel(rows, *refs),
            out_shape=(vm((n, h), BF16), vm((n, h), BF16), vm((n, f), BF16), vm((n, f), BF16),
                       vm((rows, h), F32), vm((rows, h), BF16), vm((rows, h), BF16), vm((h // 4, f), F32)),
            in_specs=[hbm] * 4,
            out_specs=(vspec,) * 8,
            scratch_shapes=[
                vm((n, f), F32),
                vm((h, f), BF16), vm((f, h), BF16), vm((f, h), BF16), vm((h, f), BF16),
                vm((n, h), F32), vm((4, rows, h), BF16), vm((4, rows, h), BF16),
                vm((3, rows, h), BF16), vm((2, rows, h), BF16),
                sem(()), sem((6,)), sem(()), sem((7,)), sem((9,)), sem((6,)), sem((4,)), pltpu.SemaphoreType.REGULAR,
            ],
            compiler_params=pltpu.CompilerParams(
                collective_id=0, has_side_effects=True, vmem_limit_bytes=40 * MIB),
            name='gather_dx',
        )(*(pltpu.with_memory_space_constraint(a, pltpu.HBM) for a in (x, dy, w1, w2)))
        mid = lax.ppermute(mid, 'tp', [(0, 1), (1, 0), (2, 4), (3, 5), (4, 2), (5, 3), (6, 7), (7, 6)])
        hops = ((0, 2), (2, 3), (3, 1), (1, 0))
        far = lax.ppermute(last, 'tp', [(2 * a + c, 2 * b + c) for a, b in hops for c in (0, 1)])
        dw1, dw2 = pl.pallas_call(
            _dw_kernel,
            out_shape=(jax.ShapeDtypeStruct((h, f), F32), jax.ShapeDtypeStruct((f, h), F32)),
            in_specs=[vspec] * 5,
            out_specs=(hbm,) * 2,
            scratch_shapes=[vm((h, f), F32), vm((f, h), F32), sem(())],
            compiler_params=pltpu.CompilerParams(vmem_limit_bytes=24 * MIB),
            cost_estimate=pl.CostEstimate(
                flops=4 * n * h * f, bytes_accessed=8 * h * f, transcendentals=0),
            name='dw',
        )(xg, dzg, zg, yg, pre)
        dx = (acc + far.astype(F32) + mid.astype(F32)).astype(BF16)
        return dx, dw1, dw2

    return jax.shard_map(
        body, mesh=mesh,
        in_specs=(P(('dp', 'tp'), None), P(('dp', 'tp'), None), P(None, 'tp'), P('tp', None)),
        out_specs=(P(('dp', 'tp'), None), P('dp', 'tp'), P(('dp', 'tp'), None)),
        check_vma=False)
```

```python
import math

import jax
import jax.numpy as jnp
from jax import lax
from jax.experimental import pallas as pl
from jax.experimental.pallas import tpu as pltpu
from jax.sharding import PartitionSpec as P


C0 = math.sqrt(2.0 / math.pi)
C1 = 0.044715
BF16 = jnp.bfloat16
F32 = jnp.float32
X, Y, Y0, Y1 = range(4)
MESH = pl.DeviceIdType.MESH
TN = (((0,), (0,)), ((), ()))
MIB = 1 << 20


def _gelu(u):
    t = jnp.tanh(C0 * (u + C1 * u * u * u))
    return 0.5 * u * (1.0 + t), 0.5 * (1.0 + t) + 0.5 * u * (1.0 - t * t) * C0 * (1.0 + 3.0 * C1 * u * u)


def _gather_kernel(rows, x_hbm, y_hbm, w1_hbm, w2_hbm,
                   xg, yg, zs, dzs, acc_ref, last_ref, mid_ref, pre_ref,
                   g1s, w1, w2, w1t, w2t, pdx, psend, precv, rsend, rrecv,
                   in_sem, w_sem, ag_send, ag_recv, ag_precv, p_recv, r_recv, met):
    t = lax.axis_index('tp')
    z, c = t // 2, t % 2
    chunk = 2 * rows
    f, h = w2.shape
    low = z < 2
    near_end, near_mid = jnp.where(low, 0, 3), jnp.where(low, 1, 2)
    far_mid, far_end = 3 - near_mid, 3 - near_end
    is_end = z == near_end
    is_mid = jnp.logical_not(is_end)
    parts = ((0, 512), (512, 512), (1024, 1024))

    def dev(chip, core):
        return {'tp': 2 * chip + core}

    def block(a, slot, core):
        r = pl.ds(pl.multiple_of(slot * chunk + core * rows, rows), rows)
        if a in (X, Y):
            return (xg, yg)[a].at[r, :]
        return yg.at[r, pl.ds((a - Y0) * (h // 2), h // 2)]

    def flag(a, slot):
        return {X: 2 * slot, Y: 2 * slot + 1, Y0: 2 * slot + 1, Y1: 8}[a]

    loads = [pltpu.make_async_copy(src, block(a, 0, c), in_sem) for a, src in ((X, x_hbm), (Y, y_hbm))]
    wloads = []
    for hbm, w, n in ((w2_hbm, w2, 4), (w1_hbm, w1, 2)):
        for i in range(n):
            r = pl.ds(i * (w.shape[0] // n), w.shape[0] // n)
            wloads.append(pltpu.make_async_copy(hbm.at[r, :], w.at[r, :], w_sem.at[len(wloads)]))
    for cp in loads:
        cp.start()

    barrier = pltpu.get_barrier_semaphore()

    def greet(chip, core):
        pl.semaphore_signal(barrier, inc=1, device_id=dev(chip, core), device_id_type=MESH)

    greet(z, 1 - c)

    @pl.when(is_end)
    def _():
        greet(near_mid, c)

    @pl.when(is_mid)
    def _():
        greet(near_end, c)
        greet(far_end, c)

    low_mid = z == 1

    @pl.when(low_mid)
    def _():
        greet(far_mid, c)

    both = xg.at[pl.ds(0, chunk), :]
    pltpu.make_async_copy(both, both, in_sem).wait()
    for cp in wloads:
        cp.start()

    @pl.when(low_mid)
    def _():
        pl.semaphore_wait(barrier, 2)

    @pl.when(jnp.logical_not(low_mid))
    def _():
        pl.semaphore_wait(barrier, 3)

    def ag_copy(a, slot, chip, to_slot):
        return pltpu.make_async_remote_copy(
            src_ref=block(a, slot, c), dst_ref=block(a, to_slot, c),
            send_sem=ag_send, recv_sem=ag_recv.at[flag(a, to_slot) - 2],
            device_id=dev(chip, c), device_id_type=MESH)

    def share(a, slot):
        return pltpu.make_async_remote_copy(
            src_ref=block(a, slot, c), dst_ref=block(a, slot, c),
            send_sem=ag_send, recv_sem=ag_precv.at[flag(a, slot)],
            device_id=dev(z, 1 - c), device_id_type=MESH)

    def end_msg(a, i):
        return ag_copy(a, 0, *((far_mid, 1), (near_mid, 3))[i])

    def mid_msg(a, i):
        return ag_copy(a, *((0, near_end, 1), (0, far_mid, 2), (1, near_end, 2), (2, near_end, 3))[i])

    def arrive(a, slot, forward=None):
        dst = block(a, slot, c)
        pltpu.make_async_copy(dst, dst, ag_recv.at[flag(a, slot) - 2]).wait()
        if forward is not None:
            mid_msg(a, forward).start()
        share(a, slot).start()

    def partner(a, slot):
        share(a, slot).wait_recv()

    def step_u(slot, m=1, half=None):
        r = pl.ds(slot * chunk, m * chunk)
        nb = f // 2

        @pl.loop(half or 0, 2 if half is None else half + 1)
        def _(n):
            s = pl.ds(pl.multiple_of(n * nb, nb), nb)
            u = jnp.dot(xg[r, :], w1[:, s], preferred_element_type=F32).astype(BF16)
            g0, g1 = _gelu(u.astype(F32))
            zs[r, s] = g0.astype(BF16)
            g1s[r, s] = g1

    def step_g(slot, m=1):
        r = pl.ds(slot * chunk, m * chunk)

        @pl.loop(0, f // 1024)
        def _(n):
            s = pl.ds(pl.multiple_of(n * 1024, 1024), 1024)
            g = jnp.dot(yg[r, :], w2t[:, s], preferred_element_type=F32)
            dzs[r, s] = (g * g1s[r, s]).astype(BF16)

    def half_g(slot, i):
        r = pl.ds(slot * chunk, chunk)
        kk = pl.ds(i * (h // 2), h // 2)

        @pl.loop(0, f // 1024)
        def _(n):
            s = pl.ds(pl.multiple_of(n * 1024, 1024), 1024)
            g = jnp.dot(yg[r, kk], w2t[kk, s], preferred_element_type=F32)
            if i == 0:
                pdx[r, s] = g
            else:
                dzs[r, s] = ((g + pdx[r, s]) * g1s[r, s]).astype(BF16)

    def step_dx(slot, m=1, half=None):
        r = pl.ds(slot * chunk, m * chunk)
        first, n, nb = (0, h // 1024, 1024) if half is None else (parts[half][0], 1, parts[half][1])

        @pl.loop(0, n)
        def _(n):
            s = pl.ds(pl.multiple_of(first + n * nb, nb if half is None else 128), nb)
            pdx[r, s] = jnp.dot(dzs[r, :], w1t[:, s], preferred_element_type=F32)
            for k in range(slot, slot + m):
                psend[k, :, s] = part(k, 1 - mine(half), s).astype(BF16)
                pair_copy(k, s, half).start()

    def first_dw():
        @pl.loop(0, pre_ref.shape[0] // 256)
        def _(n):
            s = pl.ds(pl.multiple_of(n * 256, 256), 256)
            pre_ref[s, :] = lax.dot_general(xg[:, s], dzs[...], TN, preferred_element_type=F32)

    def part(k, core, s=slice(None)):
        return pdx[pl.ds(pl.multiple_of(k * chunk + core * rows, rows), rows), s]

    def mine(half):
        return c if half is None else 1 - c

    def cols(half):
        return slice(None) if half is None else pl.ds(*parts[half])

    def pair_copy(k, s, half=None):
        return pltpu.make_async_remote_copy(
            src_ref=psend.at[k, :, s], dst_ref=precv.at[k, :, s], send_sem=ag_send,
            recv_sem=p_recv.at[3 + half if half else k],
            device_id=dev(z, 1 - c), device_id_type=MESH)

    def pair_sum(k, half=None):
        s = cols(half)
        pair_copy(k, s, half).wait_recv()
        return part(k, mine(half), s) + precv[k, :, s].astype(F32)

    def rs_copy(k, chip, i, half=None):
        s = cols(half)
        return pltpu.make_async_remote_copy(
            src_ref=rsend.at[k, :, s], dst_ref=rrecv.at[i, :, s], send_sem=ag_send,
            recv_sem=r_recv.at[1 + half if half else i],
            device_id=dev(chip, mine(half)), device_id_type=MESH)

    def rs_recv(i, half=None):
        s = cols(half)
        dst = rrecv.at[i, :, s]
        pltpu.make_async_copy(dst, dst, r_recv.at[1 + half if half else i]).wait()
        return rrecv[i, :, s].astype(F32)

    def drain(n):
        for r in (xg, yg, xg.at[pl.ds(0, (n + 12 - 16) * rows), :]):
            pltpu.make_async_copy(r, r, ag_send).wait()

    @pl.when(is_end)
    def _():
        end_msg(X, 0).start()

    @pl.when(is_mid)
    def _():
        mid_msg(X, 0).start()

        @pl.when(jnp.logical_not(low_mid))
        def _():
            pl.semaphore_signal(met, inc=1, device_id=dev(far_mid, c), device_id_type=MESH)

    share(X, 0).start()
    share(Y, 0).start()

    for i in range(4):
        wloads[i].wait()
        r = pl.ds(i * (f // 4), f // 4)
        w2t[:, r] = w2[r, :].T

    @pl.when(is_end)
    def _():
        end_msg(Y, 0).start()

    @pl.when(is_mid)
    def _():
        mid_msg(Y, 0).start()

    for i in range(8):
        if i % 4 == 0:
            wloads[4 + i // 4].wait()
        r = pl.ds(i * (h // 8), h // 8)
        w1t[:, r] = w1[r, :].T

    @pl.when(is_mid)
    def _():
        partner(X, 0)
        step_u(0)
        arrive(X, 1, forward=2)

        @pl.when(low_mid)
        def _():
            pl.semaphore_wait(met, 1)

        mid_msg(X, 1).start()

        @pl.when(low)
        def _():
            arrive(Y, 1, forward=2)
            mid_msg(Y0, 1).start()

        partner(X, 1)
        step_u(1)

        @pl.when(jnp.logical_not(low))
        def _():
            mid_msg(Y0, 1).start()
            arrive(Y, 1, forward=2)

        mid_msg(Y1, 1).start()
        partner(Y, 0)
        partner(Y, 1)
        step_g(0, 2)
        arrive(X, 2, forward=3)
        arrive(X, 3)
        step_dx(0, 2)
        arrive(Y0, 2, forward=3)
        acc_ref[...] = pair_sum(0)
        rsend[1] = pair_sum(1).astype(BF16)

        rs_copy(1, far_mid, 1).start()
        arrive(Y1, 2, forward=3)
        partner(X, 2)
        partner(X, 3)
        step_u(2, 2)
        arrive(Y, 3)
        partner(Y0, 2)
        partner(Y1, 2)
        partner(Y, 3)
        step_g(2, 2)
        step_dx(2, 2)
        first_dw()
        mid_ref[...] = pair_sum(2).astype(BF16)
        last_ref[...] = (pair_sum(3) + rs_recv(1)).astype(BF16)
        acc_ref[...] += rs_recv(0)
        drain(8 + 1)

    @pl.when(is_end)
    def _():
        partner(X, 0)
        arrive(X, 1)
        partner(X, 1)
        step_u(0, 2)
        end_msg(X, 1).start()
        arrive(Y, 1)
        partner(Y, 0)
        partner(Y, 1)
        step_g(0, 2)
        end_msg(Y, 1).start()
        step_dx(0, 2)
        arrive(X, 2)
        partner(X, 2)
        step_u(2)
        arrive(Y, 2)
        acc_ref[...] = pair_sum(0)
        rsend[1] = pair_sum(1).astype(BF16)
        rs_copy(1, near_mid, 0).start()
        partner(Y, 2)
        step_g(2)
        for i in range(len(parts)):
            step_dx(2, half=i)
        rsend[2, :, cols(0)] = pair_sum(2, 0).astype(BF16)
        rs_copy(2, far_end, 0, 0).start()
        arrive(X, 3)
        for i in range(1, len(parts)):
            rsend[2, :, cols(i)] = pair_sum(2, i).astype(BF16)
            rs_copy(2, far_end, 0, i).start()

        @pl.when(c == 1)
        def _():
            arrive(Y0, 3)
            arrive(Y1, 3)
            partner(X, 3)
            step_u(3)
            partner(Y0, 3)
            half_g(3, 0)

        @pl.when(c == 0)
        def _():
            partner(X, 3)
            step_u(3, half=0)
            arrive(Y0, 3)
            step_u(3, half=1)
            arrive(Y1, 3)
            partner(Y0, 3)
            half_g(3, 0)

        partner(Y1, 3)
        half_g(3, 1)
        step_dx(3)
        first_dw()
        mid_ref[...] = jnp.zeros_like(mid_ref)
        last_ref[...] = pair_sum(3).astype(BF16)
        for i in range(len(parts)):
            acc_ref[:, cols(i)] += rs_recv(0, i)
        drain(4 + 2)


def _dw_kernel(x, dz, zz, y, pre, dw1, dw2, b1, b2, sem):
    n = 8
    hb, fb = x.shape[1] // n, zz.shape[1] // n

    def out(j, i):
        src, dst, m = ((b1, dw1, hb), (b2, dw2, fb))[j]
        s = pl.ds(i * m, m)
        if j == 0 and (i + 1) * hb <= pre.shape[0]:
            src = pre
        return pltpu.make_async_copy(src.at[s, :], dst.at[s, :], sem)

    done = pre.shape[0] // hb
    for i in range(done):
        out(0, i).start()
    for i in range(n):
        b2[pl.ds(i * fb, fb), :] = lax.dot_general(
            zz[:, pl.ds(i * fb, fb)], y[...], TN, preferred_element_type=F32)
        out(1, i).start()
        if i >= done:
            b1[pl.ds(i * hb, hb), :] = lax.dot_general(
                x[:, pl.ds(i * hb, hb)], dz[...], TN, preferred_element_type=F32)
            out(0, i).start()
    pltpu.make_async_copy(b1, dw1, sem).wait()
    pltpu.make_async_copy(b2, dw2, sem).wait()


def solution(mesh):
    def body(x, dy, w1, w2):
        rows, h = x.shape
        f = w1.shape[1]
        n = 8 * rows
        vm = pltpu.VMEM
        sem = pltpu.SemaphoreType.DMA
        vspec = pl.BlockSpec(memory_space=vm)
        hbm = pl.BlockSpec(memory_space=pltpu.HBM)
        xg, yg, zg, dzg, acc, last, mid, pre = pl.pallas_call(
            lambda *refs: _gather_kernel(rows, *refs),
            out_shape=(vm((n, h), BF16), vm((n, h), BF16), vm((n, f), BF16), vm((n, f), BF16),
                       vm((rows, h), F32), vm((rows, h), BF16), vm((rows, h), BF16), vm((h // 4, f), F32)),
            in_specs=[hbm] * 4,
            out_specs=(vspec,) * 8,
            scratch_shapes=[
                vm((n, f), F32),
                vm((h, f), BF16), vm((f, h), BF16), vm((f, h), BF16), vm((h, f), BF16),
                vm((n, h), F32), vm((4, rows, h), BF16), vm((4, rows, h), BF16),
                vm((3, rows, h), BF16), vm((2, rows, h), BF16),
                sem(()), sem((6,)), sem(()), sem((7,)), sem((9,)), sem((6,)), sem((4,)), pltpu.SemaphoreType.REGULAR,
            ],
            compiler_params=pltpu.CompilerParams(
                collective_id=0, has_side_effects=True, vmem_limit_bytes=40 * MIB),
            name='gather_dx',
        )(*(pltpu.with_memory_space_constraint(a, pltpu.HBM) for a in (x, dy, w1, w2)))
        mid = lax.ppermute(mid, 'tp', [(0, 1), (1, 0), (2, 4), (3, 5), (4, 2), (5, 3), (6, 7), (7, 6)])
        hops = ((0, 2), (2, 3), (3, 1), (1, 0))
        far = lax.ppermute(last, 'tp', [(2 * a + c, 2 * b + c) for a, b in hops for c in (0, 1)])
        dw1, dw2 = pl.pallas_call(
            _dw_kernel,
            out_shape=(jax.ShapeDtypeStruct((h, f), F32), jax.ShapeDtypeStruct((f, h), F32)),
            in_specs=[vspec] * 5,
            out_specs=(hbm,) * 2,
            scratch_shapes=[vm((h, f), F32), vm((f, h), F32), sem(())],
            compiler_params=pltpu.CompilerParams(vmem_limit_bytes=24 * MIB),
            cost_estimate=pl.CostEstimate(
                flops=4 * n * h * f, bytes_accessed=8 * h * f, transcendentals=0),
            name='dw',
        )(xg, dzg, zg, yg, pre)
        dx = (acc + far.astype(F32) + mid.astype(F32)).astype(BF16)
        return dx, dw1, dw2

    return jax.shard_map(
        body, mesh=mesh,
        in_specs=(P(('dp', 'tp'), None), P(('dp', 'tp'), None), P(None, 'tp'), P('tp', None)),
        out_specs=(P(('dp', 'tp'), None), P('dp', 'tp'), P(('dp', 'tp'), None)),
        check_vma=False)
```

```python
import math

import jax
import jax.numpy as jnp
from jax import lax
from jax.experimental import pallas as pl
from jax.experimental.pallas import tpu as pltpu
from jax.sharding import PartitionSpec as P


C0 = math.sqrt(2.0 / math.pi)
C1 = 0.044715
BF16 = jnp.bfloat16
F32 = jnp.float32
X, Y, Y0, Y1 = range(4)
MESH = pl.DeviceIdType.MESH
TN = (((0,), (0,)), ((), ()))
MIB = 1 << 20


def _gelu(u):
    t = jnp.tanh(C0 * (u + C1 * u * u * u))
    return 0.5 * u * (1.0 + t), 0.5 * (1.0 + t) + 0.5 * u * (1.0 - t * t) * C0 * (1.0 + 3.0 * C1 * u * u)


def _gather_kernel(rows, x_hbm, y_hbm, w1_hbm, w2_hbm,
                   xg, yg, zs, dzs, acc_ref, last_ref, mid_ref, pre_ref,
                   g1s, w1, w2, w1t, w2t, pdx, psend, precv, rsend, rrecv,
                   in_sem, w_sem, ag_send, ag_recv, ag_precv, p_recv, r_recv, met):
    t = lax.axis_index('tp')
    z, c = t // 2, t % 2
    chunk = 2 * rows
    f, h = w2.shape
    low = z < 2
    near_end, near_mid = jnp.where(low, 0, 3), jnp.where(low, 1, 2)
    far_mid, far_end = 3 - near_mid, 3 - near_end
    is_end = z == near_end
    is_mid = jnp.logical_not(is_end)
    parts = ((0, 512), (512, 512), (1024, 1024))

    def dev(chip, core):
        return {'tp': 2 * chip + core}

    def block(a, slot, core):
        r = pl.ds(pl.multiple_of(slot * chunk + core * rows, rows), rows)
        if a in (X, Y):
            return (xg, yg)[a].at[r, :]
        return yg.at[r, pl.ds((a - Y0) * (h // 2), h // 2)]

    def flag(a, slot):
        return {X: 2 * slot, Y: 2 * slot + 1, Y0: 2 * slot + 1, Y1: 8}[a]

    loads = [pltpu.make_async_copy(src, block(a, 0, c), in_sem) for a, src in ((X, x_hbm), (Y, y_hbm))]
    wloads = []
    for hbm, w, n in ((w2_hbm, w2, 4), (w1_hbm, w1, 2)):
        for i in range(n):
            r = pl.ds(i * (w.shape[0] // n), w.shape[0] // n)
            wloads.append(pltpu.make_async_copy(hbm.at[r, :], w.at[r, :], w_sem.at[len(wloads)]))
    for cp in loads:
        cp.start()

    barrier = pltpu.get_barrier_semaphore()

    def greet(chip, core):
        pl.semaphore_signal(barrier, inc=1, device_id=dev(chip, core), device_id_type=MESH)

    greet(z, 1 - c)

    @pl.when(is_end)
    def _():
        greet(near_mid, c)

    @pl.when(is_mid)
    def _():
        greet(near_end, c)
        greet(far_end, c)

    low_mid = z == 1

    @pl.when(low_mid)
    def _():
        greet(far_mid, c)

    both = xg.at[pl.ds(0, chunk), :]
    pltpu.make_async_copy(both, both, in_sem).wait()
    for cp in wloads:
        cp.start()

    @pl.when(low_mid)
    def _():
        pl.semaphore_wait(barrier, 2)

    @pl.when(jnp.logical_not(low_mid))
    def _():
        pl.semaphore_wait(barrier, 3)

    def ag_copy(a, slot, chip, to_slot):
        return pltpu.make_async_remote_copy(
            src_ref=block(a, slot, c), dst_ref=block(a, to_slot, c),
            send_sem=ag_send, recv_sem=ag_recv.at[flag(a, to_slot) - 2],
            device_id=dev(chip, c), device_id_type=MESH)

    def share(a, slot):
        return pltpu.make_async_remote_copy(
            src_ref=block(a, slot, c), dst_ref=block(a, slot, c),
            send_sem=ag_send, recv_sem=ag_precv.at[flag(a, slot)],
            device_id=dev(z, 1 - c), device_id_type=MESH)

    def end_msg(a, i):
        return ag_copy(a, 0, *((far_mid, 1), (near_mid, 3))[i])

    def mid_msg(a, i):
        return ag_copy(a, *((0, near_end, 1), (0, far_mid, 2), (1, near_end, 2), (2, near_end, 3))[i])

    def arrive(a, slot, forward=None):
        dst = block(a, slot, c)
        pltpu.make_async_copy(dst, dst, ag_recv.at[flag(a, slot) - 2]).wait()
        if forward is not None:
            mid_msg(a, forward).start()
        share(a, slot).start()

    def partner(a, slot):
        share(a, slot).wait_recv()

    def step_u(slot, m=1, half=None):
        r = pl.ds(slot * chunk, m * chunk)
        nb = f // 2

        @pl.loop(half or 0, 2 if half is None else half + 1)
        def _(n):
            s = pl.ds(pl.multiple_of(n * nb, nb), nb)
            u = jnp.dot(xg[r, :], w1[:, s], preferred_element_type=F32).astype(BF16)
            g0, g1 = _gelu(u.astype(F32))
            zs[r, s] = g0.astype(BF16)
            g1s[r, s] = g1

    def step_g(slot, m=1):
        r = pl.ds(slot * chunk, m * chunk)

        @pl.loop(0, f // 1024)
        def _(n):
            s = pl.ds(pl.multiple_of(n * 1024, 1024), 1024)
            g = jnp.dot(yg[r, :], w2t[:, s], preferred_element_type=F32)
            dzs[r, s] = (g * g1s[r, s]).astype(BF16)

    def half_g(slot, i):
        r = pl.ds(slot * chunk, chunk)
        kk = pl.ds(i * (h // 2), h // 2)

        @pl.loop(0, f // 1024)
        def _(n):
            s = pl.ds(pl.multiple_of(n * 1024, 1024), 1024)
            g = jnp.dot(yg[r, kk], w2t[kk, s], preferred_element_type=F32)
            if i == 0:
                pdx[r, s] = g
            else:
                dzs[r, s] = ((g + pdx[r, s]) * g1s[r, s]).astype(BF16)

    def step_dx(slot, m=1, half=None):
        r = pl.ds(slot * chunk, m * chunk)
        first, n, nb = (0, h // 1024, 1024) if half is None else (parts[half][0], 1, parts[half][1])

        @pl.loop(0, n)
        def _(n):
            s = pl.ds(pl.multiple_of(first + n * nb, nb if half is None else 128), nb)
            pdx[r, s] = jnp.dot(dzs[r, :], w1t[:, s], preferred_element_type=F32)
            for k in range(slot, slot + m):
                psend[k, :, s] = part(k, 1 - mine(half), s).astype(BF16)
                pair_copy(k, s, half).start()

    def first_dw():
        @pl.loop(0, pre_ref.shape[0] // 256)
        def _(n):
            s = pl.ds(pl.multiple_of(n * 256, 256), 256)
            pre_ref[s, :] = lax.dot_general(xg[:, s], dzs[...], TN, preferred_element_type=F32)

    def part(k, core, s=slice(None)):
        return pdx[pl.ds(pl.multiple_of(k * chunk + core * rows, rows), rows), s]

    def mine(half):
        return c if half is None else 1 - c

    def cols(half):
        return slice(None) if half is None else pl.ds(*parts[half])

    def pair_copy(k, s, half=None):
        return pltpu.make_async_remote_copy(
            src_ref=psend.at[k, :, s], dst_ref=precv.at[k, :, s], send_sem=ag_send,
            recv_sem=p_recv.at[3 + half if half else k],
            device_id=dev(z, 1 - c), device_id_type=MESH)

    def pair_sum(k, half=None):
        s = cols(half)
        pair_copy(k, s, half).wait_recv()
        return part(k, mine(half), s) + precv[k, :, s].astype(F32)

    def rs_copy(k, chip, i, half=None):
        s = cols(half)
        return pltpu.make_async_remote_copy(
            src_ref=rsend.at[k, :, s], dst_ref=rrecv.at[i, :, s], send_sem=ag_send,
            recv_sem=r_recv.at[1 + half if half else i],
            device_id=dev(chip, mine(half)), device_id_type=MESH)

    def rs_recv(i, half=None):
        s = cols(half)
        dst = rrecv.at[i, :, s]
        pltpu.make_async_copy(dst, dst, r_recv.at[1 + half if half else i]).wait()
        return rrecv[i, :, s].astype(F32)

    def drain(n):
        for r in (xg, yg, xg.at[pl.ds(0, (n + 12 - 16) * rows), :]):
            pltpu.make_async_copy(r, r, ag_send).wait()

    @pl.when(is_end)
    def _():
        end_msg(X, 0).start()

    @pl.when(is_mid)
    def _():
        mid_msg(X, 0).start()

        @pl.when(jnp.logical_not(low_mid))
        def _():
            pl.semaphore_signal(met, inc=1, device_id=dev(far_mid, c), device_id_type=MESH)

    share(X, 0).start()
    share(Y, 0).start()

    for i in range(4):
        wloads[i].wait()
        r = pl.ds(i * (f // 4), f // 4)
        w2t[:, r] = w2[r, :].T

    @pl.when(is_end)
    def _():
        end_msg(Y, 0).start()

    @pl.when(is_mid)
    def _():
        mid_msg(Y, 0).start()

    for i in range(8):
        if i % 4 == 0:
            wloads[4 + i // 4].wait()
        r = pl.ds(i * (h // 8), h // 8)
        w1t[:, r] = w1[r, :].T

    @pl.when(is_mid)
    def _():
        partner(X, 0)
        step_u(0)
        arrive(X, 1, forward=2)

        @pl.when(low_mid)
        def _():
            pl.semaphore_wait(met, 1)

        mid_msg(X, 1).start()

        @pl.when(low)
        def _():
            arrive(Y, 1, forward=2)
            mid_msg(Y0, 1).start()

        partner(X, 1)
        step_u(1)

        @pl.when(jnp.logical_not(low))
        def _():
            mid_msg(Y0, 1).start()
            arrive(Y, 1, forward=2)

        mid_msg(Y1, 1).start()
        partner(Y, 0)
        partner(Y, 1)
        step_g(0, 2)
        arrive(X, 2, forward=3)
        arrive(X, 3)
        step_dx(0, 2)
        arrive(Y0, 2, forward=3)
        acc_ref[...] = pair_sum(0)
        rsend[1] = pair_sum(1).astype(BF16)

        rs_copy(1, far_mid, 1).start()
        arrive(Y1, 2, forward=3)
        partner(X, 2)
        partner(X, 3)
        step_u(2, 2)
        arrive(Y, 3)
        partner(Y0, 2)
        partner(Y1, 2)
        partner(Y, 3)
        step_g(2, 2)
        step_dx(2, 2)
        first_dw()
        mid_ref[...] = pair_sum(2).astype(BF16)
        last_ref[...] = (pair_sum(3) + rs_recv(1)).astype(BF16)
        acc_ref[...] += rs_recv(0)
        drain(8 + 1)

    @pl.when(is_end)
    def _():
        partner(X, 0)
        arrive(X, 1)
        partner(X, 1)
        step_u(0, 2)
        end_msg(X, 1).start()
        arrive(Y, 1)
        partner(Y, 0)
        partner(Y, 1)
        step_g(0, 2)
        end_msg(Y, 1).start()
        step_dx(0, 2)
        arrive(X, 2)
        partner(X, 2)
        step_u(2)
        arrive(Y, 2)
        acc_ref[...] = pair_sum(0)
        rsend[1] = pair_sum(1).astype(BF16)
        rs_copy(1, near_mid, 0).start()
        partner(Y, 2)
        step_g(2)
        for i in range(len(parts)):
            step_dx(2, half=i)
        rsend[2, :, cols(0)] = pair_sum(2, 0).astype(BF16)
        rs_copy(2, far_end, 0, 0).start()
        arrive(X, 3)
        for i in range(1, len(parts)):
            rsend[2, :, cols(i)] = pair_sum(2, i).astype(BF16)
            rs_copy(2, far_end, 0, i).start()

        @pl.when(c == 1)
        def _():
            arrive(Y0, 3)
            arrive(Y1, 3)
            partner(X, 3)
            step_u(3)
            partner(Y0, 3)
            half_g(3, 0)

        @pl.when(c == 0)
        def _():
            partner(X, 3)
            step_u(3, half=0)
            arrive(Y0, 3)
            step_u(3, half=1)
            arrive(Y1, 3)
            partner(Y0, 3)
            half_g(3, 0)

        partner(Y1, 3)
        half_g(3, 1)
        step_dx(3)
        first_dw()
        mid_ref[...] = jnp.zeros_like(mid_ref)
        last_ref[...] = pair_sum(3).astype(BF16)
        for i in range(len(parts)):
            acc_ref[:, cols(i)] += rs_recv(0, i)
        drain(4 + 2)


def _dw_kernel(x, dz, zz, y, pre, dw1, dw2, b1, b2, sem):
    n = 8
    hb, fb = x.shape[1] // n, zz.shape[1] // n

    def out(j, i):
        src, dst, m = ((b1, dw1, hb), (b2, dw2, fb))[j]
        s = pl.ds(i * m, m)
        if j == 0 and (i + 1) * hb <= pre.shape[0]:
            src = pre
        return pltpu.make_async_copy(src.at[s, :], dst.at[s, :], sem)

    done = pre.shape[0] // hb
    for i in range(done):
        out(0, i).start()
    for i in range(n):
        b2[pl.ds(i * fb, fb), :] = lax.dot_general(
            zz[:, pl.ds(i * fb, fb)], y[...], TN, preferred_element_type=F32)
        out(1, i).start()
        if i >= done:
            b1[pl.ds(i * hb, hb), :] = lax.dot_general(
                x[:, pl.ds(i * hb, hb)], dz[...], TN, preferred_element_type=F32)
            out(0, i).start()
    pltpu.make_async_copy(b1, dw1, sem).wait()
    pltpu.make_async_copy(b2, dw2, sem).wait()


def _add_kernel(acc, far, mid, dx, buf, sem):
    half = acc.shape[0] // 2
    for i in range(2):
        r = pl.ds(i * half, half)
        buf[r, :] = (acc[r, :] + far[r, :].astype(F32) + mid[r, :].astype(F32)).astype(BF16)
        pltpu.make_async_copy(buf.at[r, :], dx.at[r, :], sem).start()
    pltpu.make_async_copy(buf, dx, sem).wait()


def solution(mesh):
    def body(x, dy, w1, w2):
        rows, h = x.shape
        f = w1.shape[1]
        n = 8 * rows
        vm = pltpu.VMEM
        sem = pltpu.SemaphoreType.DMA
        vspec = pl.BlockSpec(memory_space=vm)
        hbm = pl.BlockSpec(memory_space=pltpu.HBM)
        xg, yg, zg, dzg, acc, last, mid, pre = pl.pallas_call(
            lambda *refs: _gather_kernel(rows, *refs),
            out_shape=(vm((n, h), BF16), vm((n, h), BF16), vm((n, f), BF16), vm((n, f), BF16),
                       vm((rows, h), F32), vm((rows, h), BF16), vm((rows, h), BF16), vm((h // 4, f), F32)),
            in_specs=[hbm] * 4,
            out_specs=(vspec,) * 8,
            scratch_shapes=[
                vm((n, f), F32),
                vm((h, f), BF16), vm((f, h), BF16), vm((f, h), BF16), vm((h, f), BF16),
                vm((n, h), F32), vm((4, rows, h), BF16), vm((4, rows, h), BF16),
                vm((3, rows, h), BF16), vm((2, rows, h), BF16),
                sem(()), sem((6,)), sem(()), sem((7,)), sem((9,)), sem((6,)), sem((4,)), pltpu.SemaphoreType.REGULAR,
            ],
            compiler_params=pltpu.CompilerParams(
                collective_id=0, has_side_effects=True, vmem_limit_bytes=40 * MIB),
            name='gather_dx',
        )(*(pltpu.with_memory_space_constraint(a, pltpu.HBM) for a in (x, dy, w1, w2)))
        mid = lax.ppermute(mid, 'tp', [(0, 1), (1, 0), (2, 4), (3, 5), (4, 2), (5, 3), (6, 7), (7, 6)])
        hops = ((0, 2), (2, 3), (3, 1), (1, 0))
        far = lax.ppermute(last, 'tp', [(2 * a + c, 2 * b + c) for a, b in hops for c in (0, 1)])
        dw1, dw2 = pl.pallas_call(
            _dw_kernel,
            out_shape=(jax.ShapeDtypeStruct((h, f), F32), jax.ShapeDtypeStruct((f, h), F32)),
            in_specs=[vspec] * 5,
            out_specs=(hbm,) * 2,
            scratch_shapes=[vm((h, f), F32), vm((f, h), F32), sem(())],
            compiler_params=pltpu.CompilerParams(vmem_limit_bytes=24 * MIB),
            cost_estimate=pl.CostEstimate(
                flops=4 * n * h * f, bytes_accessed=8 * h * f, transcendentals=0),
            name='dw',
        )(xg, dzg, zg, yg, pre)
        dx = pl.pallas_call(
            _add_kernel,
            out_shape=jax.ShapeDtypeStruct((rows, h), BF16),
            in_specs=[vspec] * 3,
            out_specs=hbm,
            scratch_shapes=[vm((rows, h), BF16), sem(())],
            compiler_params=pltpu.CompilerParams(vmem_limit_bytes=2 * MIB),
            name='add',
        )(acc, far, mid)
        return dx, dw1, dw2

    return jax.shard_map(
        body, mesh=mesh,
        in_specs=(P(('dp', 'tp'), None), P(('dp', 'tp'), None), P(None, 'tp'), P('tp', None)),
        out_specs=(P(('dp', 'tp'), None), P('dp', 'tp'), P(('dp', 'tp'), None)),
        check_vma=False)
```
